256 devices in a mesh: batch: 4 (over x_lo, core), seq: 64 (over y, x_hi, z).
Axes of the slice: x: 4 (x_hi: 2, x_lo: 2; x = x_hi * 2 + x_lo), y: 4, z: 8, core: 2. Of those that a mesh axis runs over, the one named last changes fastest.
Arguments:
- signal: bfloat16 [4, 16384, 256], P('batch', 'seq'), may hold values from -0.125 to 0.125
- grad_out: bfloat16 [4, 16384, 256], P('batch', 'seq'), may hold values from -6 to 6
- filter_taps: float32 [16384, 256], P('seq'), may hold values from -0.125 to 0.125
- skip_gain: float32 [256], replicated, may hold values from 0.5 to 2
Outputs:
- input_grad: bfloat16 [4, 16384, 256], P('batch', 'seq')
- filter_grad: float32 [16384, 256], P('seq')
The draws below stay inside these ranges and needn't reach their ends.
All inputs are finite; a program needn't handle non-finite values.
Results may differ from the reference program's by a relative error of at most 0.001.
Values sent between devices are 32-bit elements; how exact they have to be, the bound alone decides.
No kernel may reach another device: no remote copies, remote signals or barrier semaphores. Data moves between devices by JAX's collectives and lax.ppermute only.
A program may use at most 64 MiB of HBM per device.

```python
import jax
import jax.numpy as jnp

CHANNELS = 256
LENGTH = 16384
BATCH = 4


def levels(stream_key, dims, pieces, least, high):
    factor_of, own = 1.0, jax.random.fold_in(stream_key, 6)
    for dim, blocks in pieces:
        heights = jnp.exp(jax.random.uniform(jax.random.fold_in(own, dim), (blocks,), jnp.float32, least / len(pieces), high / len(pieces)))
        factor_of = factor_of * jnp.repeat(heights, dims[dim] // blocks).reshape([-1 if axis == dim else 1 for axis in range(len(dims))])
    return factor_of


def scatter_about(own_key, dims, width, bound, shards=(), dtype=jnp.bfloat16):
    array = width * jax.random.normal(own_key, dims, jnp.float32)
    if shards:
        array = array * levels(own_key, dims, shards, -0.22, 0.18)
    return jnp.clip(array, -bound, bound).astype(dtype)


def setup_inputs(seed: int = 0) -> dict:
    keys = jax.random.split(jax.random.key(seed), 5)
    return {
        "signal": scatter_about(keys[0], (BATCH, LENGTH, CHANNELS), (LENGTH ** -0.5), 0.125, ((0, 4), (1, 64))),
        "grad_out": scatter_about(keys[1], (BATCH, LENGTH, CHANNELS), 1.0, 6.0, ((0, 4), (1, 64))),
        "filter_taps": scatter_about(keys[2], (LENGTH, CHANNELS), (LENGTH ** -0.5), 0.125, ((0, 64),), jnp.float32),
        "skip_gain": jnp.clip(jax.random.uniform(keys[3], (CHANNELS,), jnp.float32, 0.5, 2.0), 0.5, 2.0),
    }


def reference(signal, grad_out, filter_taps, skip_gain):
    length = signal.shape[1]
    padded_len = 2 * length
    signal_full = signal.astype(jnp.float32)
    grad_full = grad_out.astype(jnp.float32)
    signal_spec = jnp.fft.rfft(signal_full, n=padded_len, axis=1)
    grad_spec = jnp.fft.rfft(grad_full, n=padded_len, axis=1)
    taps_spec = jnp.fft.rfft(filter_taps, n=padded_len, axis=0)
    input_conv = jnp.fft.irfft(grad_spec * jnp.conj(taps_spec)[None], n=padded_len, axis=1)[:, :length]
    input_grad = (input_conv + skip_gain[None, None, :] * grad_full).astype(jnp.bfloat16)
    summed = jnp.sum(grad_spec * jnp.conj(signal_spec), axis=0)
    filter_grad = jnp.fft.irfft(summed, n=padded_len, axis=0)[:length]
    return input_grad, filter_grad.astype(jnp.float32)
```

```python
import functools

import jax
import jax.numpy as jnp
from jax import lax
from jax.experimental import pallas as pl
from jax.experimental.pallas import tpu as pltpu
from jax.sharding import PartitionSpec as P

LANES = 128
BLOCK = 256


def anti_identity(size):
    row = lax.broadcasted_iota(jnp.int32, (size, size), 0)
    column = lax.broadcasted_iota(jnp.int32, (size, size), 1)
    return jnp.where(row + column == size - 1, 1.0, 0.0).astype(jnp.bfloat16)


def product(left, right):
    return jnp.dot(left, right, preferred_element_type=jnp.float32)


def correlate(batch, blocks, got_ref, out_ref, hankel, flipped, u_left, h_left, total):
    tile = 5
    per_batch = BLOCK // batch
    flip_rows = anti_identity(blocks)
    flip_lanes = anti_identity(LANES)

    def rows_of(b, part):
        return got_ref[pl.ds(b * blocks * tile + part, blocks, stride=tile), :]

    def reversed_rows(values):
        turned = product(flip_rows, values.astype(jnp.bfloat16)).astype(jnp.bfloat16)
        return product(turned, flip_lanes)

    def spread(kind, left, base):
        for offset in range(16):
            for half in range(2):
                count = 2 * blocks - 16
                left[offset, base : base + count, half * LANES : (half + 1) * LANES] = flipped[
                    kind, half, pl.ds(offset, count), :
                ].astype(jnp.bfloat16)

    flipped[...] = jnp.zeros_like(flipped)
    halves = BLOCK // LANES
    pieces = LANES // per_batch
    for half in range(halves):
        taps = jnp.concatenate(
            [rows_of(half * pieces + piece, 4)[:, :per_batch] for piece in range(pieces)], axis=1
        )
        high = taps.astype(jnp.bfloat16).astype(jnp.float32)
        flipped[1, half, 0:blocks, :] = reversed_rows(high)
        flipped[2, half, 0:blocks, :] = reversed_rows(taps - high)
    count = 2 * blocks - 16
    spread(1, h_left, 0)
    spread(2, h_left, count)

    hankel[pl.ds(2 * blocks * LANES, LANES), :] = jnp.zeros((LANES, LANES), jnp.bfloat16)
    row = lax.broadcasted_iota(jnp.int32, (LANES, LANES), 0)
    lane = lax.broadcasted_iota(jnp.int32, (LANES, LANES), 1)
    own = lane <= row

    def turned(b, block):
        values = got_ref[pl.ds((b * blocks + block // 2) * tile + 2 + block % 2, 1), :]
        return pltpu.roll(jnp.broadcast_to(values, (LANES, LANES)), 1, 1, stride=1, stride_axis=0)

    def one_batch(b, carry):
        for half in range(halves):
            flipped[0, half, 0:blocks, :] = reversed_rows(rows_of(b, half))
        spread(0, u_left, 0)

        def build(step, current):
            for inner in range(2):
                block = 2 * step + inner
                following = turned(b, block + 1)
                hankel[pl.ds(block * LANES, LANES), :] = jnp.where(own, current, following).astype(
                    jnp.bfloat16
                )
                current = following
            return current

        current = lax.fori_loop(0, blocks - 1, build, turned(b, 0))
        block = 2 * blocks - 2
        following = turned(b, block + 1)
        hankel[pl.ds(block * LANES, LANES), :] = jnp.where(own, current, following).astype(
            jnp.bfloat16
        )
        hankel[pl.ds((block + 1) * LANES, LANES), :] = jnp.where(own, following, 0.0).astype(
            jnp.bfloat16
        )

        total[1] = jnp.zeros((blocks, BLOCK), jnp.float32)
        for group in range(blocks // 16):
            height = 16 * (group + 1)
            result = None
            for inner in range(16):
                k = 16 * group + inner
                start = blocks - 1 - k
                offset, base = start % 16, start - start % 16
                left = jnp.concatenate(
                    [
                        u_left[offset, base : base + height, :],
                        h_left[offset, base : base + height, :],
                        h_left[offset, count + base : count + base + height, :],
                    ],
                    axis=0,
                )
                right = jnp.concatenate(
                    [
                        hankel[k * BLOCK : (k + 1) * BLOCK, :],
                        hankel[k * BLOCK + LANES : (k + 1) * BLOCK + LANES, :],
                    ],
                    axis=1,
                )
                term = product(left, right)
                result = term if result is None else result + term
            total[0, 0:height, :] += result[0:height]
            total[1, 0:height, :] += result[height : 2 * height] + result[2 * height :]
        for half in range(halves):
            out_ref[pl.ds(b * blocks, blocks), half, :] = total[
                1, :, half * LANES : (half + 1) * LANES
            ]
        return carry

    total[0] = jnp.zeros((blocks, BLOCK), jnp.float32)
    lax.fori_loop(0, batch, one_batch, 0)
    for b in range(batch):
        for half in range(halves):
            out_ref[b * blocks : (b + 1) * blocks, 2 + half, :] = total[
                0, :, half * LANES : (half + 1) * LANES
            ]


def correlations(got, batch, blocks):
    count = 2 * blocks - 16
    return pl.pallas_call(
        functools.partial(correlate, batch, blocks),
        out_shape=jax.ShapeDtypeStruct((batch * blocks, 4, LANES), jnp.float32),
        in_specs=[pl.BlockSpec(memory_space=pltpu.VMEM)],
        out_specs=pl.BlockSpec(memory_space=pltpu.VMEM),
        scratch_shapes=[
            pltpu.VMEM(((2 * blocks + 1) * LANES, LANES), jnp.bfloat16),
            pltpu.VMEM((3, 2, 2 * blocks, LANES), jnp.float32),
            pltpu.VMEM((16, count, BLOCK), jnp.bfloat16),
            pltpu.VMEM((16, 2 * count, BLOCK), jnp.bfloat16),
            pltpu.VMEM((2, blocks, BLOCK), jnp.float32),
        ],
        cost_estimate=pl.CostEstimate(flops=6_000_000_000, bytes_accessed=2_000_000, transcendentals=0),
        name="correlate",
    )(got)


def shards(signal, grad_out, filter_taps, skip_gain):
    batch, blocks = lax.axis_size("batch"), lax.axis_size("seq")
    axes = ("batch", "seq")
    channels = filter_taps.shape[1]
    per_batch = BLOCK // batch
    grad_rows = grad_out[0].astype(jnp.float32)
    signal_rows = signal[0].astype(jnp.float32)
    taps = lax.dynamic_slice_in_dim(filter_taps, lax.axis_index("batch") * per_batch, per_batch, 0)
    sent = jnp.concatenate(
        [signal_rows.T, grad_rows.T, taps.T, jnp.zeros((channels, LANES - per_batch), jnp.float32)],
        axis=1,
    ).reshape(channels, 5, 1, LANES)
    got = lax.all_to_all(sent, axes, 0, 0, tiled=True)
    back = correlations(got.reshape(5 * channels, LANES), batch, blocks)
    home = lax.all_to_all(back, axes, 0, 0, tiled=True)
    input_conv = home[:, 0:2, :].reshape(channels, BLOCK).T
    filter_grad = home[:, 2:4, :].reshape(channels, BLOCK).T
    input_grad = (input_conv + skip_gain[None, :] * grad_rows).astype(jnp.bfloat16)
    return (input_grad[None], filter_grad)


def solution(mesh):
    return jax.shard_map(
        shards,
        mesh=mesh,
        in_specs=(P("batch", "seq", None), P("batch", "seq", None), P("seq", None), P()),
        out_specs=(P("batch", "seq", None), P("seq", None)),
        check_vma=False,
    )
```

```python
import functools

import jax
import jax.numpy as jnp
from jax import lax
from jax.experimental import pallas as pl
from jax.experimental.pallas import tpu as pltpu
from jax.sharding import PartitionSpec as P

LANES = 128
BLOCK = 256
PACK = 16


def anti_identity(size):
    row = lax.broadcasted_iota(jnp.int32, (size, size), 0)
    column = lax.broadcasted_iota(jnp.int32, (size, size), 1)
    return jnp.where(row + column == size - 1, 1.0, 0.0).astype(jnp.bfloat16)


def product(left, right):
    return jnp.dot(left, right, preferred_element_type=jnp.float32)


def correlate(batch, blocks, got_ref, out_ref, even, odd, flipped, u_left, h_left, total):
    tile = 5
    halves = BLOCK // LANES
    groups = blocks // PACK
    per_batch = BLOCK // batch
    flip_rows = anti_identity(blocks)
    flip_lanes = anti_identity(LANES)
    row = lax.broadcasted_iota(jnp.int32, (LANES, LANES), 0)
    lane = lax.broadcasted_iota(jnp.int32, (LANES, LANES), 1)
    nothing = jnp.zeros((LANES, LANES), jnp.float32)

    def rows_of(b, part):
        return got_ref[pl.ds(b * blocks * tile + part, blocks, stride=tile), :]

    def reversed_rows(values):
        turned = product(flip_rows, values.astype(jnp.bfloat16)).astype(jnp.bfloat16)
        return product(turned, flip_lanes)

    def spread(kind, left, base):
        for offset in range(PACK):
            for half in range(halves):
                left[offset, base : base + blocks, half * LANES : (half + 1) * LANES] = flipped[
                    kind, half, pl.ds(offset, blocks), :
                ].astype(jnp.bfloat16)

    def turned(b, block):
        values = got_ref[pl.ds((b * blocks + block // 2) * tile + 2 + block % 2, 1), :]
        return pltpu.roll(jnp.broadcast_to(values, (LANES, LANES)), 1, 1, stride=1, stride_axis=0)

    def build(b, group, hankel):
        count = 2 * PACK + 1
        first = 2 * PACK * group

        def at(block):
            return turned(b, block) if block < 2 * blocks else nothing

        current = at(first)
        for inner in range(count):
            following = at(first + inner + 1)
            hankel[inner * LANES : (inner + 1) * LANES, :] = jnp.where(
                lane <= row, current, following
            ).astype(jnp.bfloat16)
            current = following

    def multiply(group, hankel):
        height = PACK * (group + 1)
        base = blocks - height
        result = None
        for inner in range(PACK):
            offset = PACK - 1 - inner
            left = jnp.concatenate(
                [
                    u_left[offset, base:blocks, :],
                    h_left[offset, base:blocks, :],
                    h_left[offset, blocks + base : 2 * blocks, :],
                ],
                axis=0,
            )
            right = jnp.concatenate(
                [
                    hankel[inner * BLOCK : (inner + 1) * BLOCK, :],
                    hankel[inner * BLOCK + LANES : (inner + 1) * BLOCK + LANES, :],
                ],
                axis=1,
            )
            term = product(left, right)
            result = term if result is None else result + term
        total[0, 0:height, :] += result[0:height]
        total[1, 0:height, :] += result[height : 2 * height] + result[2 * height :]

    flipped[...] = jnp.zeros_like(flipped)
    pieces = LANES // per_batch
    for half in range(halves):
        taps = jnp.concatenate(
            [rows_of(half * pieces + piece, 4)[:, :per_batch] for piece in range(pieces)], axis=1
        )
        high = taps.astype(jnp.bfloat16).astype(jnp.float32)
        flipped[batch, half, 0:blocks, :] = reversed_rows(high)
        flipped[batch + 1, half, 0:blocks, :] = reversed_rows(taps - high)
        for b in range(batch):
            flipped[b, half, 0:blocks, :] = reversed_rows(rows_of(b, half))
    spread(batch, h_left, 0)
    spread(batch + 1, h_left, blocks)
    total[0] = jnp.zeros((blocks, BLOCK), jnp.float32)
    build(0, 0, even)

    def one_batch(b, carry):
        total[1] = jnp.zeros((blocks, BLOCK), jnp.float32)
        spread(b, u_left, 0)
        for group in range(groups):
            now, later = (even, odd) if group % 2 == 0 else (odd, even)
            if group + 1 < groups:
                build(b, group + 1, later)
            else:
                build(jnp.minimum(b + 1, batch - 1), 0, later)
            multiply(group, now)
        for half in range(halves):
            out_ref[pl.ds(b * blocks * 4 + half, blocks, stride=4), :] = total[
                1, :, half * LANES : (half + 1) * LANES
            ]
        return carry

    lax.fori_loop(0, batch, one_batch, 0)
    for b in range(batch):
        for half in range(halves):
            out_ref[pl.ds(b * blocks * 4 + 2 + half, blocks, stride=4), :] = total[
                0, :, half * LANES : (half + 1) * LANES
            ]


def correlations(got, batch, blocks):
    hankel = pltpu.VMEM(((2 * PACK + 1) * LANES, LANES), jnp.bfloat16)
    return pl.pallas_call(
        functools.partial(correlate, batch, blocks),
        out_shape=jax.ShapeDtypeStruct((batch * blocks * 4, LANES), jnp.float32),
        in_specs=[pl.BlockSpec(memory_space=pltpu.VMEM)],
        out_specs=pl.BlockSpec(memory_space=pltpu.VMEM),
        scratch_shapes=[
            hankel,
            hankel,
            pltpu.VMEM((batch + 2, 2, blocks + PACK, LANES), jnp.float32),
            pltpu.VMEM((PACK, blocks, BLOCK), jnp.bfloat16),
            pltpu.VMEM((PACK, 2 * blocks, BLOCK), jnp.bfloat16),
            pltpu.VMEM((2, blocks, BLOCK), jnp.float32),
        ],
        compiler_params=pltpu.CompilerParams(vmem_limit_bytes=24 * 1024 * 1024),
        cost_estimate=pl.CostEstimate(flops=6_000_000_000, bytes_accessed=2_000_000, transcendentals=0),
        name="correlate",
    )(got)


def shards(signal, grad_out, filter_taps, skip_gain):
    batch, blocks = lax.axis_size("batch"), lax.axis_size("seq")
    axes = ("batch", "seq")
    channels = filter_taps.shape[1]
    per_batch = BLOCK // batch
    grad_rows = grad_out[0].astype(jnp.float32)
    signal_rows = signal[0].astype(jnp.float32)
    taps = lax.dynamic_slice_in_dim(filter_taps, lax.axis_index("batch") * per_batch, per_batch, 0)
    sent = jnp.concatenate(
        [signal_rows.T, grad_rows.T, taps.T, jnp.zeros((channels, LANES - per_batch), jnp.float32)],
        axis=1,
    ).reshape(channels, 5, 1, LANES)
    got = lax.all_to_all(sent, axes, 0, 0, tiled=True)
    back = correlations(got.reshape(5 * channels, LANES), batch, blocks).reshape(channels, 4, LANES)
    home = lax.all_to_all(back, axes, 0, 0, tiled=True)
    input_conv = home[:, 0:2, :].reshape(channels, BLOCK).T
    filter_grad = home[:, 2:4, :].reshape(channels, BLOCK).T
    input_grad = (input_conv + skip_gain[None, :] * grad_rows).astype(jnp.bfloat16)
    return (input_grad[None], filter_grad)


def solution(mesh):
    return jax.shard_map(
        shards,
        mesh=mesh,
        in_specs=(P("batch", "seq", None), P("batch", "seq", None), P("seq", None), P()),
        out_specs=(P("batch", "seq", None), P("seq", None)),
        check_vma=False,
    )
```

```python
import functools

import jax
import jax.numpy as jnp
from jax import lax
from jax.experimental import pallas as pl
from jax.experimental.pallas import tpu as pltpu
from jax.sharding import PartitionSpec as P

LANES = 128
ROWS = 8
BLOCK = 256
HALVES = BLOCK // LANES
PACK = 16
SENT = 5
BACK = 4


def product(left, right):
    return jnp.dot(left, right, preferred_element_type=jnp.float32)


def anti_identity(size):
    row = lax.broadcasted_iota(jnp.int32, (size, size), 0)
    column = lax.broadcasted_iota(jnp.int32, (size, size), 1)
    return jnp.where(row + column == size - 1, 1.0, 0.0).astype(jnp.bfloat16)


def correlate(batch, blocks, got_ref, out_ref, even, odd, flipped, h_left, total):
    groups = blocks // PACK
    per_batch = BLOCK // batch
    flip_lanes = anti_identity(LANES)
    row = lax.broadcasted_iota(jnp.int32, (LANES, LANES), 0)
    lane = lax.broadcasted_iota(jnp.int32, (LANES, LANES), 1)
    nothing = jnp.zeros((LANES, LANES), jnp.float32)
    gain = jnp.broadcast_to(got_ref[SENT - 1 : SENT, per_batch : per_batch + 1], (1, LANES))
    upward = ROWS - 1 - lax.broadcasted_iota(jnp.int32, (ROWS, LANES), 0)

    def rows_of(b, part):
        return got_ref[pl.ds(b * blocks * SENT + part, blocks, stride=SENT), :]

    def keep_flipped(kind, half, values):
        turned = product(values.astype(jnp.bfloat16), flip_lanes)
        for first in range(0, blocks, ROWS):
            flipped[kind, half, blocks - ROWS - first : blocks - first, :] = jnp.take_along_axis(
                turned[first : first + ROWS], upward, axis=0
            )
        flipped[kind, half, blocks : blocks + PACK, :] = jnp.zeros((PACK, LANES), jnp.float32)

    def spread(kind, left, base):
        for offset in range(PACK):
            for half in range(HALVES):
                left[offset, base : base + blocks, half * LANES : (half + 1) * LANES] = flipped[
                    kind, half, pl.ds(offset, blocks), :
                ].astype(jnp.bfloat16)

    def turned(b, block):
        values = got_ref[pl.ds((b * blocks + block // 2) * SENT + HALVES + block % 2, 1), :]
        return pltpu.roll(jnp.broadcast_to(values, (LANES, LANES)), 1, 1, stride=1, stride_axis=0)

    def build(b, group, hankel):
        count = 2 * PACK + 1
        first = 2 * PACK * group

        def at(block):
            return turned(b, block) if block < 2 * blocks else nothing

        current = at(first)
        for inner in range(count):
            following = at(first + inner + 1)
            hankel[inner * LANES : (inner + 1) * LANES, :] = jnp.where(
                lane <= row, current, following
            ).astype(jnp.bfloat16)
            current = following

    def multiply(b, group, hankel):
        height = PACK * (group + 1)
        base = blocks - height
        result = None
        for inner in range(PACK):
            offset = PACK - 1 - inner
            own = [
                flipped[b, half, pl.ds(base + offset, height), :].astype(jnp.bfloat16)
                for half in range(HALVES)
            ]
            left = jnp.concatenate(
                [
                    jnp.concatenate(own, axis=1),
                    h_left[offset, base:blocks, :],
                    h_left[offset, blocks + base : 2 * blocks, :],
                ],
                axis=0,
            )
            right = jnp.concatenate(
                [
                    hankel[inner * BLOCK : (inner + 1) * BLOCK, :],
                    hankel[inner * BLOCK + LANES : (inner + 1) * BLOCK + LANES, :],
                ],
                axis=1,
            )
            term = product(left, right)
            result = term if result is None else result + term
        total[0, 0:height, :] += result[0:height]
        total[1, 0:height, :] += result[height : 2 * height] + result[2 * height :]

    build(0, 0, even)
    pieces = LANES // per_batch
    for half in range(HALVES):
        taps = jnp.concatenate(
            [rows_of(half * pieces + piece, SENT - 1)[:, :per_batch] for piece in range(pieces)],
            axis=1,
        )
        high = taps.astype(jnp.bfloat16).astype(jnp.float32)
        keep_flipped(batch, half, high)
        keep_flipped(batch + 1, half, taps - high)
        for b in range(batch):
            keep_flipped(b, half, rows_of(b, half))
    spread(batch, h_left, 0)
    spread(batch + 1, h_left, blocks)
    total[0] = jnp.zeros((blocks, BLOCK), jnp.float32)

    def one_batch(b, last):
        total[1] = jnp.zeros((blocks, BLOCK), jnp.float32)
        for group in range(groups):
            now, later = (even, odd) if group % 2 == 0 else (odd, even)
            if group + 1 < groups:
                build(b, group + 1, later)
            elif not last:
                build(b + 1, 0, later)
            multiply(b, group, now)
        for half in range(HALVES):
            out_ref[pl.ds(b * blocks * BACK + half, blocks, stride=BACK), :] = (
                total[1, :, half * LANES : (half + 1) * LANES]
                + gain * rows_of(b, HALVES + half)
            )

    def step(b, carry):
        one_batch(b, False)
        return carry

    lax.fori_loop(0, batch - 1, step, 0)
    one_batch(batch - 1, True)
    for b in range(batch):
        for half in range(HALVES):
            out_ref[pl.ds(b * blocks * BACK + HALVES + half, blocks, stride=BACK), :] = total[
                0, :, half * LANES : (half + 1) * LANES
            ]


def correlations(got, batch, blocks):
    hankel = pltpu.VMEM(((2 * PACK + 1) * LANES, LANES), jnp.bfloat16)
    return pl.pallas_call(
        functools.partial(correlate, batch, blocks),
        out_shape=jax.ShapeDtypeStruct((batch * blocks * BACK, LANES), jnp.float32),
        in_specs=[pl.BlockSpec(memory_space=pltpu.VMEM)],
        out_specs=pl.BlockSpec(memory_space=pltpu.VMEM),
        scratch_shapes=[
            hankel,
            hankel,
            pltpu.VMEM((batch + 2, HALVES, blocks + PACK, LANES), jnp.float32),
            pltpu.VMEM((PACK, 2 * blocks, BLOCK), jnp.bfloat16),
            pltpu.VMEM((2, blocks, BLOCK), jnp.float32),
        ],
        compiler_params=pltpu.CompilerParams(vmem_limit_bytes=24 * 1024 * 1024),
        cost_estimate=pl.CostEstimate(flops=6_000_000_000, bytes_accessed=2_000_000, transcendentals=0),
        name="correlate",
    )(got)


def finish(home_ref, input_ref, filter_ref, own, shared, left):
    channels = filter_ref.shape[1]
    copies = []

    def send_home(source, target):
        copies.append(pltpu.make_async_copy(source, target, left.at[len(copies)]))
        copies[-1].start()

    for half in range(HALVES):
        rows = slice(half * LANES, (half + 1) * LANES)
        shared[rows, :] = home_ref[pl.ds(HALVES + half, channels, stride=BACK), :].T
        send_home(shared.at[rows, :], filter_ref.at[rows, :])
    for half in range(HALVES):
        rows = slice(half * LANES, (half + 1) * LANES)
        conv = home_ref[pl.ds(half, channels, stride=BACK), :].T
        own[0, rows, :] = conv.astype(jnp.bfloat16)
        send_home(own.at[:, rows, :], input_ref.at[:, rows, :])
    for copy in copies:
        copy.wait()


def gradients(home):
    channels = home.shape[0] // BACK
    vmem = pl.BlockSpec(memory_space=pltpu.VMEM)
    hbm = pl.BlockSpec(memory_space=pltpu.HBM)
    return pl.pallas_call(
        finish,
        out_shape=(
            jax.ShapeDtypeStruct((1, BLOCK, channels), jnp.bfloat16),
            jax.ShapeDtypeStruct((BLOCK, channels), jnp.float32),
        ),
        in_specs=[vmem],
        out_specs=(hbm, hbm),
        scratch_shapes=[
            pltpu.VMEM((1, BLOCK, channels), jnp.bfloat16),
            pltpu.VMEM((BLOCK, channels), jnp.float32),
            pltpu.SemaphoreType.DMA((2 * HALVES,)),
        ],
        compiler_params=pltpu.CompilerParams(vmem_limit_bytes=16 * 1024 * 1024),
        name="finish",
    )(home)


def shards(signal, grad_out, filter_taps, skip_gain):
    batch, blocks = lax.axis_size("batch"), lax.axis_size("seq")
    axes = ("batch", "seq")
    channels = filter_taps.shape[1]
    per_batch = BLOCK // batch
    grad_rows = grad_out[0].astype(jnp.float32)
    signal_rows = signal[0].astype(jnp.float32)
    gain = jnp.broadcast_to(skip_gain[:, None], (channels, LANES - per_batch))
    taps = lax.dynamic_slice_in_dim(filter_taps, lax.axis_index("batch") * per_batch, per_batch, 0)
    sent = jnp.concatenate(
        [signal_rows.T, grad_rows.T, taps.T, gain], axis=1
    ).reshape(channels, SENT, 1, LANES)
    got = lax.all_to_all(sent, axes, 0, 0, tiled=True)
    back = correlations(got.reshape(channels * SENT, LANES), batch, blocks)
    home = lax.all_to_all(back.reshape(channels, BACK, LANES), axes, 0, 0, tiled=True)
    return gradients(home.reshape(channels * BACK, LANES))


def solution(mesh):
    return jax.shard_map(
        shards,
        mesh=mesh,
        in_specs=(P("batch", "seq", None), P("batch", "seq", None), P("seq", None), P()),
        out_specs=(P("batch", "seq", None), P("seq", None)),
        check_vma=False,
    )
```

```python
import functools

import jax
import jax.numpy as jnp
from jax import lax
from jax.experimental import pallas as pl
from jax.experimental.pallas import tpu as pltpu
from jax.sharding import PartitionSpec as P

LANES = 128
ROWS = 8
BLOCK = 256
HALVES = BLOCK // LANES
PACK = 16
SENT = 5
BACK = 3


def product(left, right):
    return jnp.dot(left, right, preferred_element_type=jnp.float32)


def anti_identity(size):
    row = lax.broadcasted_iota(jnp.int32, (size, size), 0)
    column = lax.broadcasted_iota(jnp.int32, (size, size), 1)
    return jnp.where(row + column == size - 1, 1.0, 0.0).astype(jnp.bfloat16)


def correlate(batch, blocks, got_ref, out_ref, even, odd, flipped, h_left, total):
    groups = blocks // PACK
    per_batch = BLOCK // batch
    flip_lanes = anti_identity(LANES)
    row = lax.broadcasted_iota(jnp.int32, (LANES, LANES), 0)
    lane = lax.broadcasted_iota(jnp.int32, (LANES, LANES), 1)
    nothing = jnp.zeros((LANES, LANES), jnp.float32)
    gain = jnp.broadcast_to(got_ref[SENT - 1 : SENT, per_batch : per_batch + 1], (1, LANES))
    upward = ROWS - 1 - lax.broadcasted_iota(jnp.int32, (ROWS, LANES), 0)

    def rows_of(b, part):
        return got_ref[pl.ds(b * blocks * SENT + part, blocks, stride=SENT), :]

    def keep_flipped(kind, half, values):
        turned = product(values.astype(jnp.bfloat16), flip_lanes)
        for first in range(0, blocks, ROWS):
            flipped[kind, half, blocks - ROWS - first : blocks - first, :] = jnp.take_along_axis(
                turned[first : first + ROWS], upward, axis=0
            )
        flipped[kind, half, blocks : blocks + PACK, :] = jnp.zeros((PACK, LANES), jnp.float32)

    def spread(kind, left, base):
        for offset in range(PACK):
            for half in range(HALVES):
                left[offset, base : base + blocks, half * LANES : (half + 1) * LANES] = flipped[
                    kind, half, pl.ds(offset, blocks), :
                ].astype(jnp.bfloat16)

    def turned(b, block):
        values = got_ref[pl.ds((b * blocks + block // 2) * SENT + HALVES + block % 2, 1), :]
        return pltpu.roll(jnp.broadcast_to(values, (LANES, LANES)), 1, 1, stride=1, stride_axis=0)

    def build(b, group, hankel):
        count = 2 * PACK + 1
        first = 2 * PACK * group

        def at(block):
            return turned(b, block) if block < 2 * blocks else nothing

        current = at(first)
        for inner in range(count):
            following = at(first + inner + 1)
            hankel[inner * LANES : (inner + 1) * LANES, :] = jnp.where(
                lane <= row, current, following
            ).astype(jnp.bfloat16)
            current = following

    def multiply(b, group, hankel):
        height = PACK * (group + 1)
        base = blocks - height
        result = None
        for inner in range(PACK):
            offset = PACK - 1 - inner
            own = [
                flipped[b, half, pl.ds(base + offset, height), :].astype(jnp.bfloat16)
                for half in range(HALVES)
            ]
            left = jnp.concatenate(
                [
                    jnp.concatenate(own, axis=1),
                    h_left[offset, base:blocks, :],
                    h_left[offset, blocks + base : 2 * blocks, :],
                ],
                axis=0,
            )
            right = jnp.concatenate(
                [
                    hankel[inner * BLOCK : (inner + 1) * BLOCK, :],
                    hankel[inner * BLOCK + LANES : (inner + 1) * BLOCK + LANES, :],
                ],
                axis=1,
            )
            term = product(left, right)
            result = term if result is None else result + term
        total[0, 0:height, :] += result[0:height]
        total[1, 0:height, :] += result[height : 2 * height] + result[2 * height :]

    build(0, 0, even)
    pieces = LANES // per_batch
    for half in range(HALVES):
        taps = jnp.concatenate(
            [rows_of(half * pieces + piece, SENT - 1)[:, :per_batch] for piece in range(pieces)],
            axis=1,
        )
        high = taps.astype(jnp.bfloat16).astype(jnp.float32)
        keep_flipped(batch, half, high)
        keep_flipped(batch + 1, half, taps - high)
        for b in range(batch):
            keep_flipped(b, half, rows_of(b, half))
    spread(batch, h_left, 0)
    spread(batch + 1, h_left, blocks)
    total[0] = jnp.zeros((blocks, BLOCK), jnp.float32)

    def one_batch(b, last):
        total[1] = jnp.zeros((blocks, BLOCK), jnp.float32)
        for group in range(groups):
            now, later = (even, odd) if group % 2 == 0 else (odd, even)
            if group + 1 < groups:
                build(b, group + 1, later)
            elif not last:
                build(b + 1, 0, later)
            multiply(b, group, now)
        for half in range(HALVES):
            out_ref[pl.ds(b * blocks * BACK + half, blocks, stride=BACK), :] = (
                total[1, :, half * LANES : (half + 1) * LANES]
                + gain * rows_of(b, HALVES + half)
            )

    def step(b, carry):
        one_batch(b, False)
        return carry

    lax.fori_loop(0, batch - 1, step, 0)
    one_batch(batch - 1, True)
    for b in range(batch):
        half = b % HALVES
        out_ref[pl.ds(b * blocks * BACK + HALVES, blocks, stride=BACK), :] = total[
            0, :, half * LANES : (half + 1) * LANES
        ]


def correlations(got, batch, blocks):
    hankel = pltpu.VMEM(((2 * PACK + 1) * LANES, LANES), jnp.bfloat16)
    return pl.pallas_call(
        functools.partial(correlate, batch, blocks),
        out_shape=jax.ShapeDtypeStruct((batch * blocks * BACK, LANES), jnp.float32),
        in_specs=[pl.BlockSpec(memory_space=pltpu.VMEM)],
        out_specs=pl.BlockSpec(memory_space=pltpu.VMEM),
        scratch_shapes=[
            hankel,
            hankel,
            pltpu.VMEM((batch + 2, HALVES, blocks + PACK, LANES), jnp.float32),
            pltpu.VMEM((PACK, 2 * blocks, BLOCK), jnp.bfloat16),
            pltpu.VMEM((2, blocks, BLOCK), jnp.float32),
        ],
        compiler_params=pltpu.CompilerParams(vmem_limit_bytes=24 * 1024 * 1024),
        cost_estimate=pl.CostEstimate(flops=6_000_000_000, bytes_accessed=2_000_000, transcendentals=0),
        name="correlate",
    )(got)


def write_out(pairs, left):
    copies = [
        pltpu.make_async_copy(source, target, left.at[place])
        for place, (source, target) in enumerate(pairs)
    ]
    for copy in copies:
        copy.start()
    return copies


def turn(home_ref, half_ref):
    channels = half_ref.shape[1]
    half_ref[...] = home_ref[pl.ds(HALVES, channels, stride=BACK), :].T


def filter_half(home):
    channels = home.shape[0] // BACK
    vmem = pl.BlockSpec(memory_space=pltpu.VMEM)
    return pl.pallas_call(
        turn,
        out_shape=jax.ShapeDtypeStruct((LANES, channels), jnp.float32),
        in_specs=[vmem],
        out_specs=vmem,
        compiler_params=pltpu.CompilerParams(vmem_limit_bytes=16 * 1024 * 1024),
        name="turn",
    )(home)


def finish(home_ref, input_ref, own, left):
    channels = input_ref.shape[2]
    copies = []
    for half in range(HALVES):
        rows = slice(half * LANES, (half + 1) * LANES)
        conv = home_ref[pl.ds(half, channels, stride=BACK), :].T
        own[0, rows, :] = conv.astype(jnp.bfloat16)
        copies += write_out([(own.at[:, rows, :], input_ref.at[:, rows, :])], left.at[pl.ds(half, 1)])
    for copy in copies:
        copy.wait()


def input_gradient(home):
    channels = home.shape[0] // BACK
    return pl.pallas_call(
        finish,
        out_shape=jax.ShapeDtypeStruct((1, BLOCK, channels), jnp.bfloat16),
        in_specs=[pl.BlockSpec(memory_space=pltpu.VMEM)],
        out_specs=pl.BlockSpec(memory_space=pltpu.HBM),
        scratch_shapes=[
            pltpu.VMEM((1, BLOCK, channels), jnp.bfloat16),
            pltpu.SemaphoreType.DMA((HALVES,)),
        ],
        compiler_params=pltpu.CompilerParams(vmem_limit_bytes=16 * 1024 * 1024),
        cost_estimate=pl.CostEstimate(flops=1_000_000_000, bytes_accessed=1_000_000, transcendentals=0),
        name="finish",
    )(home)


def join(own_ref, other_ref, filter_ref, left):
    core = lax.rem(lax.axis_index("batch"), HALVES)
    copies = write_out(
        [
            (own_ref, filter_ref.at[pl.ds(pl.multiple_of(core * LANES, LANES), LANES), :]),
            (other_ref, filter_ref.at[pl.ds(pl.multiple_of((1 - core) * LANES, LANES), LANES), :]),
        ],
        left,
    )
    for copy in copies:
        copy.wait()


def filter_gradient(own, other):
    vmem = pl.BlockSpec(memory_space=pltpu.VMEM)
    return pl.pallas_call(
        join,
        out_shape=jax.ShapeDtypeStruct((BLOCK, own.shape[1]), jnp.float32),
        in_specs=[vmem, vmem],
        out_specs=pl.BlockSpec(memory_space=pltpu.HBM),
        scratch_shapes=[pltpu.SemaphoreType.DMA((HALVES,))],
        compiler_params=pltpu.CompilerParams(vmem_limit_bytes=16 * 1024 * 1024),
        name="join",
    )(own, other)


def shards(signal, grad_out, filter_taps, skip_gain):
    batch, blocks = lax.axis_size("batch"), lax.axis_size("seq")
    axes = ("batch", "seq")
    channels = filter_taps.shape[1]
    per_batch = BLOCK // batch
    grad_rows = grad_out[0].astype(jnp.float32)
    signal_rows = signal[0].astype(jnp.float32)
    gain = jnp.broadcast_to(skip_gain[:, None], (channels, LANES - per_batch))
    signal_rows, grad_rows, gain = lax.optimization_barrier((signal_rows, grad_rows, gain))
    taps = lax.dynamic_slice_in_dim(filter_taps, lax.axis_index("batch") * per_batch, per_batch, 0)
    sent = jnp.concatenate(
        [signal_rows.T, grad_rows.T, taps.T, gain], axis=1
    ).reshape(channels, SENT, 1, LANES)
    got = lax.all_to_all(sent, axes, 0, 0, tiled=True)
    back = correlations(got.reshape(channels * SENT, LANES), batch, blocks)
    home = lax.all_to_all(back.reshape(channels, BACK, 1, LANES), axes, 0, 0, tiled=True)
    home = home.reshape(channels * BACK, LANES)
    own = filter_half(home)
    other = lax.ppermute(own, "batch", [(b, b ^ 1) for b in range(batch)])
    return (input_gradient(home), filter_gradient(own, other))


def solution(mesh):
    return jax.shard_map(
        shards,
        mesh=mesh,
        in_specs=(P("batch", "seq", None), P("batch", "seq", None), P("seq", None), P()),
        out_specs=(P("batch", "seq", None), P("seq", None)),
        check_vma=False,
    )
```

```python
import functools

import jax
import jax.numpy as jnp
from jax import lax
from jax.experimental import pallas as pl
from jax.experimental.pallas import tpu as pltpu
from jax.sharding import PartitionSpec as P

LANES = 128
ROWS = 8
BLOCK = 256
HALVES = BLOCK // LANES
SENT = 5
BACK = 3


def product(left, right):
    return jnp.dot(left, right, preferred_element_type=jnp.float32)


def send(per_batch, signal_ref, grad_ref, taps_ref, gain_ref, sent_ref):
    channels = gain_ref.shape[1]
    for half in range(HALVES):
        rows = slice(half * LANES, (half + 1) * LANES)
        sent_ref[pl.ds(half, channels, stride=SENT), :] = signal_ref[rows, :].T
        sent_ref[pl.ds(HALVES + half, channels, stride=SENT), :] = grad_ref[rows, :].T
    first = pl.multiple_of(lax.axis_index("batch") * per_batch, per_batch)
    taps = taps_ref[pl.ds(first, per_batch), :]
    sent_ref[pl.ds(SENT - 1, channels, stride=SENT), :] = jnp.concatenate(
        [taps, gain_ref[...]], axis=0
    ).T


def pieces_to_send(signal_rows, grad_rows, filter_taps, gain, per_batch):
    channels = gain.shape[1]
    vmem = pl.BlockSpec(memory_space=pltpu.VMEM)
    return pl.pallas_call(
        functools.partial(send, per_batch),
        out_shape=jax.ShapeDtypeStruct((channels * SENT, LANES), jnp.float32),
        in_specs=[vmem] * 4,
        out_specs=vmem,
        compiler_params=pltpu.CompilerParams(vmem_limit_bytes=16 * 1024 * 1024),
        name="send",
    )(signal_rows, grad_rows, filter_taps, gain)


def correlate(batch, blocks, got_ref, out_ref, even, odd, ordered, total):
    turns = blocks // 2
    groups = turns // ROWS
    per_batch = BLOCK // batch
    window = LANES // 2
    gain = jnp.broadcast_to(got_ref[SENT - 1 : SENT, per_batch : per_batch + 1], (1, LANES))
    row = lax.broadcasted_iota(jnp.int32, (window, LANES), 0)
    lane = lax.broadcasted_iota(jnp.int32, (window, LANES), 1)
    own = lane <= 2 * row + 1
    nothing = jnp.zeros((window, LANES), jnp.float32)
    source = lax.broadcasted_iota(jnp.int32, (BLOCK, BLOCK), 0)
    target = lax.broadcasted_iota(jnp.int32, (BLOCK, BLOCK), 1)
    step = source // 2
    place = LANES * (source % 2) + window * (step // window) + (window - 1 - step % window)
    lanes_to = jnp.where(place == target, 1.0, 0.0).astype(jnp.bfloat16)
    target = lax.broadcasted_iota(jnp.int32, (blocks, blocks), 0)
    source = lax.broadcasted_iota(jnp.int32, (blocks, blocks), 1)
    place = turns * (source % 2) + (turns - 1 - source // 2)
    rows_to = jnp.where(place == target, 1.0, 0.0).astype(jnp.bfloat16)

    def rows_of(b, part):
        return got_ref[pl.ds(b * blocks * SENT + part, blocks, stride=SENT), :]

    def put_in_order(kind, halves):
        values = jnp.concatenate(halves, axis=1).astype(jnp.bfloat16)
        moved = product(rows_to, product(values, lanes_to).astype(jnp.bfloat16))
        for parity in range(2):
            for side in range(2):
                ordered[kind, parity, side, 0:turns, :] = moved[
                    side * turns : (side + 1) * turns, parity * LANES : (parity + 1) * LANES
                ]
                ordered[kind, parity, side, turns : turns + ROWS, :] = jnp.zeros(
                    (ROWS, LANES), jnp.float32
                )

    def turned(b, block):
        values = got_ref[pl.ds((b * blocks + block // 2) * SENT + HALVES + block % 2, 1), :]
        return pltpu.roll(jnp.broadcast_to(values, (window, LANES)), 2, 1, stride=2, stride_axis=0)

    def build(b, group, hankel):
        first = 4 * ROWS * group

        def at(block):
            return turned(b, block) if block < 2 * blocks else nothing

        current = at(first)
        for inner in range(4 * ROWS + 3):
            following = at(first + inner + 1)
            hankel[inner * window : (inner + 1) * window, :] = jnp.where(
                own, current, following
            ).astype(jnp.bfloat16)
            current = following

    def multiply(b, group, hankel):
        height = ROWS * (group + 1)
        base = turns - height
        result = None
        for inner in range(ROWS):
            start = base + ROWS - 1 - inner
            left = jnp.concatenate(
                [
                    jnp.concatenate(
                        [ordered[kind, parity, side, pl.ds(start, height), :] for side in range(2)],
                        axis=1,
                    )
                    for kind in (b, batch, batch + 1)
                    for parity in range(2)
                ],
                axis=0,
            ).astype(jnp.bfloat16)
            right = jnp.concatenate(
                [
                    hankel[(4 * inner + part) * window : (4 * inner + part) * window + BLOCK, :]
                    for part in range(4)
                ],
                axis=1,
            )
            term = product(left, right)
            result = term if result is None else result + term
        for parity in range(2):
            part = result[parity * height : (parity + 1) * height]
            high = result[(2 + parity) * height : (3 + parity) * height]
            low = result[(4 + parity) * height : (5 + parity) * height]
            for run in range(4):
                lanes = slice(run * LANES, (run + 1) * LANES)
                total[batch, parity, run, 0:height, :] += part[:, lanes]
                if group == 0:
                    total[b, parity, run, 0:height, :] = high[:, lanes] + low[:, lanes]
                    total[b, parity, run, height : turns + ROWS, :] = jnp.zeros(
                        (turns + ROWS - height, LANES), jnp.float32
                    )
                else:
                    total[b, parity, run, 0:height, :] += high[:, lanes] + low[:, lanes]

    build(0, 0, even)
    pieces = LANES // per_batch
    taps = [
        jnp.concatenate(
            [rows_of(half * pieces + piece, SENT - 1)[:, :per_batch] for piece in range(pieces)],
            axis=1,
        )
        for half in range(HALVES)
    ]
    high = [half.astype(jnp.bfloat16).astype(jnp.float32) for half in taps]
    put_in_order(batch, high)
    put_in_order(batch + 1, [half - part for half, part in zip(taps, high)])
    for b in range(batch):
        put_in_order(b, [rows_of(b, half) for half in range(HALVES)])
    total[batch] = jnp.zeros(total.shape[1:], jnp.float32)

    def one_batch(b, last):
        for group in range(groups):
            now, later = (even, odd) if group % 2 == 0 else (odd, even)
            if group + 1 < groups:
                build(b, group + 1, later)
            elif not last:
                build(b + 1, 0, later)
            multiply(b, group, now)

    def one_step(b, carry):
        one_batch(b, False)
        return carry

    lax.fori_loop(0, batch - 1, one_step, 0)
    one_batch(batch - 1, True)

    last_lane = lax.broadcasted_iota(jnp.int32, (turns, LANES), 1) == LANES - 1
    for kind in range(batch + 1):
        late = [pltpu.roll(total[kind, 1, run, 0:turns, :], LANES - 1, 1) for run in range(4)]
        late.append(pltpu.roll(total[kind, 1, 0, 1 : turns + 1, :], LANES - 1, 1))
        for run in range(4):
            side, half = run // 2, run % 2
            joined = total[kind, 0, run, 0:turns, :] + jnp.where(
                last_lane, late[run + 1], late[run]
            )
            if kind < batch:
                place = (kind * blocks + side) * SENT + HALVES + half
                joined = joined + gain * got_ref[pl.ds(place, turns, stride=2 * SENT), :]
                out_ref[pl.ds((kind * blocks + side) * BACK + half, turns, stride=2 * BACK), :] = joined
            else:
                for b in range(half, batch, HALVES):
                    place = (b * blocks + side) * BACK + HALVES
                    out_ref[pl.ds(place, turns, stride=2 * BACK), :] = joined


def correlations(got, batch, blocks):
    turns = blocks // 2
    hankel = pltpu.VMEM(((4 * ROWS + 3) * LANES // 2, LANES), jnp.bfloat16)
    return pl.pallas_call(
        functools.partial(correlate, batch, blocks),
        out_shape=jax.ShapeDtypeStruct((batch * blocks * BACK, LANES), jnp.float32),
        in_specs=[pl.BlockSpec(memory_space=pltpu.VMEM)],
        out_specs=pl.BlockSpec(memory_space=pltpu.VMEM),
        scratch_shapes=[
            hankel,
            hankel,
            pltpu.VMEM((batch + 2, 2, 2, turns + ROWS, LANES), jnp.float32),
            pltpu.VMEM((batch + 1, 2, 4, turns + ROWS, LANES), jnp.float32),
        ],
        compiler_params=pltpu.CompilerParams(vmem_limit_bytes=24 * 1024 * 1024),
        cost_estimate=pl.CostEstimate(flops=6_000_000_000, bytes_accessed=2_000_000, transcendentals=0),
        name="correlate",
    )(got)


def write_out(pairs, left):
    copies = [
        pltpu.make_async_copy(source, target, left.at[place])
        for place, (source, target) in enumerate(pairs)
    ]
    for copy in copies:
        copy.start()
    return copies


def turn(home_ref, half_ref):
    channels = half_ref.shape[1]
    half_ref[...] = home_ref[pl.ds(HALVES, channels, stride=BACK), :].T


def filter_half(home):
    channels = home.shape[0] // BACK
    vmem = pl.BlockSpec(memory_space=pltpu.VMEM)
    return pl.pallas_call(
        turn,
        out_shape=jax.ShapeDtypeStruct((LANES, channels), jnp.float32),
        in_specs=[vmem],
        out_specs=vmem,
        compiler_params=pltpu.CompilerParams(vmem_limit_bytes=16 * 1024 * 1024),
        name="turn",
    )(home)


def finish(home_ref, input_ref, own, left):
    channels = input_ref.shape[2]
    copies = []
    for half in range(HALVES):
        rows = slice(half * LANES, (half + 1) * LANES)
        conv = home_ref[pl.ds(half, channels, stride=BACK), :].T
        own[0, rows, :] = conv.astype(jnp.bfloat16)
        copies += write_out([(own.at[:, rows, :], input_ref.at[:, rows, :])], left.at[pl.ds(half, 1)])
    for copy in copies:
        copy.wait()


def input_gradient(home):
    channels = home.shape[0] // BACK
    return pl.pallas_call(
        finish,
        out_shape=jax.ShapeDtypeStruct((1, BLOCK, channels), jnp.bfloat16),
        in_specs=[pl.BlockSpec(memory_space=pltpu.VMEM)],
        out_specs=pl.BlockSpec(memory_space=pltpu.HBM),
        scratch_shapes=[
            pltpu.VMEM((1, BLOCK, channels), jnp.bfloat16),
            pltpu.SemaphoreType.DMA((HALVES,)),
        ],
        compiler_params=pltpu.CompilerParams(vmem_limit_bytes=16 * 1024 * 1024),
        cost_estimate=pl.CostEstimate(flops=1_000_000_000, bytes_accessed=1_000_000, transcendentals=0),
        name="finish",
    )(home)


def join(own_ref, other_ref, filter_ref, left):
    core = lax.rem(lax.axis_index("batch"), HALVES)
    copies = write_out(
        [
            (own_ref, filter_ref.at[pl.ds(pl.multiple_of(core * LANES, LANES), LANES), :]),
            (other_ref, filter_ref.at[pl.ds(pl.multiple_of((1 - core) * LANES, LANES), LANES), :]),
        ],
        left,
    )
    for copy in copies:
        copy.wait()


def filter_gradient(own, other):
    vmem = pl.BlockSpec(memory_space=pltpu.VMEM)
    return pl.pallas_call(
        join,
        out_shape=jax.ShapeDtypeStruct((BLOCK, own.shape[1]), jnp.float32),
        in_specs=[vmem, vmem],
        out_specs=pl.BlockSpec(memory_space=pltpu.HBM),
        scratch_shapes=[pltpu.SemaphoreType.DMA((HALVES,))],
        compiler_params=pltpu.CompilerParams(vmem_limit_bytes=16 * 1024 * 1024),
        name="join",
    )(own, other)


def shards(signal, grad_out, filter_taps, skip_gain):
    batch, blocks = lax.axis_size("batch"), lax.axis_size("seq")
    axes = ("batch", "seq")
    channels = filter_taps.shape[1]
    grad_rows = grad_out[0].astype(jnp.float32)
    signal_rows = signal[0].astype(jnp.float32)
    per_batch = BLOCK // batch
    gain = jnp.broadcast_to(skip_gain[None, :], (LANES - per_batch, channels))
    signal_rows, grad_rows, gain = lax.optimization_barrier((signal_rows, grad_rows, gain))
    sent = pieces_to_send(signal_rows, grad_rows, filter_taps, gain, per_batch)
    sent = sent.reshape(channels, SENT, 1, LANES)
    got = lax.all_to_all(sent, axes, 0, 0, tiled=True)
    back = correlations(got.reshape(channels * SENT, LANES), batch, blocks)
    home = lax.all_to_all(back.reshape(channels, BACK, 1, LANES), axes, 0, 0, tiled=True)
    home = home.reshape(channels * BACK, LANES)
    own = filter_half(home)
    other = lax.ppermute(own, "batch", [(b, b ^ 1) for b in range(batch)])
    return (input_gradient(home), filter_gradient(own, other))


def solution(mesh):
    return jax.shard_map(
        shards,
        mesh=mesh,
        in_specs=(P("batch", "seq", None), P("batch", "seq", None), P("seq", None), P()),
        out_specs=(P("batch", "seq", None), P("seq", None)),
        check_vma=False,
    )
```

```python
import functools

import jax
import jax.numpy as jnp
from jax import lax
from jax.experimental import pallas as pl
from jax.experimental.pallas import tpu as pltpu
from jax.sharding import PartitionSpec as P

LANES = 128
ROWS = 8
BLOCK = 256
HALVES = BLOCK // LANES
PACK = 16
SENT = 5
BACK = 3


def product(left, right):
    return jnp.dot(left, right, preferred_element_type=jnp.float32)


def send(per_batch, signal_ref, grad_ref, taps_ref, gain_ref, sent_ref):
    channels = gain_ref.shape[1]
    for half in range(HALVES):
        rows = slice(half * LANES, (half + 1) * LANES)
        sent_ref[pl.ds(half, channels, stride=SENT), :] = signal_ref[rows, :].T
        sent_ref[pl.ds(HALVES + half, channels, stride=SENT), :] = grad_ref[rows, :].T
    first = pl.multiple_of(lax.axis_index("batch") * per_batch, per_batch)
    taps = taps_ref[pl.ds(first, per_batch), :]
    sent_ref[pl.ds(SENT - 1, channels, stride=SENT), :] = jnp.concatenate(
        [taps, gain_ref[...]], axis=0
    ).T


def pieces_to_send(signal_rows, grad_rows, filter_taps, gain, per_batch):
    channels = gain.shape[1]
    vmem = pl.BlockSpec(memory_space=pltpu.VMEM)
    return pl.pallas_call(
        functools.partial(send, per_batch),
        out_shape=jax.ShapeDtypeStruct((channels * SENT, LANES), jnp.float32),
        in_specs=[vmem] * 4,
        out_specs=vmem,
        compiler_params=pltpu.CompilerParams(vmem_limit_bytes=16 * 1024 * 1024),
        name="send",
    )(signal_rows, grad_rows, filter_taps, gain)


def correlate(batch, blocks, got_ref, out_ref, even, odd, ordered, total):
    groups = blocks // PACK
    per_batch = BLOCK // batch
    window = LANES // 2
    gain = jnp.broadcast_to(got_ref[SENT - 1 : SENT, per_batch : per_batch + 1], (1, LANES))
    row = lax.broadcasted_iota(jnp.int32, (window, LANES), 0)
    lane = lax.broadcasted_iota(jnp.int32, (window, LANES), 1)
    own = lane <= 2 * row + 1
    nothing = jnp.zeros((window, LANES), jnp.float32)
    source = lax.broadcasted_iota(jnp.int32, (BLOCK, BLOCK), 0)
    target = lax.broadcasted_iota(jnp.int32, (BLOCK, BLOCK), 1)
    step = source // 2
    place = LANES * (source % 2) + window * (step // window) + (window - 1 - step % window)
    lanes_to = jnp.where(place == target, 1.0, 0.0).astype(jnp.bfloat16)
    target = lax.broadcasted_iota(jnp.int32, (blocks, blocks), 0)
    source = lax.broadcasted_iota(jnp.int32, (blocks, blocks), 1)
    rows_to = jnp.where(source + target == blocks - 1, 1.0, 0.0).astype(jnp.bfloat16)

    def rows_of(b, part):
        return got_ref[pl.ds(b * blocks * SENT + part, blocks, stride=SENT), :]

    def put_in_order(kind, halves):
        values = jnp.concatenate(halves, axis=1).astype(jnp.bfloat16)
        moved = product(rows_to, product(values, lanes_to).astype(jnp.bfloat16))
        for parity in range(2):
            ordered[kind, parity, 0:blocks, :] = moved[:, parity * LANES : (parity + 1) * LANES]
            ordered[kind, parity, blocks : blocks + PACK, :] = jnp.zeros((PACK, LANES), jnp.float32)

    def turned(b, block):
        values = got_ref[pl.ds((b * blocks + block // 2) * SENT + HALVES + block % 2, 1), :]
        return pltpu.roll(jnp.broadcast_to(values, (window, LANES)), 2, 1, stride=2, stride_axis=0)

    def build(b, group, hankel):
        first = 2 * PACK * group

        def at(block):
            return turned(b, block) if block < 2 * blocks else nothing

        current = at(first)
        for inner in range(2 * PACK + 3):
            following = at(first + inner + 1)
            hankel[inner * window : (inner + 1) * window, :] = jnp.where(
                own, current, following
            ).astype(jnp.bfloat16)
            current = following

    def multiply(b, group, hankel):
        height = PACK * (group + 1)
        base = blocks - height
        result = None
        for inner in range(PACK // 2):
            start = base + PACK - 1 - 2 * inner
            left = jnp.concatenate(
                [
                    jnp.concatenate(
                        [
                            ordered[kind, parity, pl.ds(start - later, height), :]
                            for later in range(2)
                        ],
                        axis=1,
                    )
                    for kind in (b, batch, batch + 1)
                    for parity in range(2)
                ],
                axis=0,
            ).astype(jnp.bfloat16)
            right = jnp.concatenate(
                [
                    hankel[(4 * inner + half) * window : (4 * inner + half) * window + BLOCK, :]
                    for half in range(HALVES)
                ],
                axis=1,
            )
            term = product(left, right)
            result = term if result is None else result + term
        for parity in range(2):
            part = result[parity * height : (parity + 1) * height]
            high = result[(2 + parity) * height : (3 + parity) * height]
            low = result[(4 + parity) * height : (5 + parity) * height]
            for half in range(HALVES):
                lanes = slice(half * LANES, (half + 1) * LANES)
                total[batch, parity, half, 0:height, :] += part[:, lanes]
                if group == 0:
                    total[b, parity, half, 0:height, :] = high[:, lanes] + low[:, lanes]
                    total[b, parity, half, height : blocks + ROWS, :] = jnp.zeros(
                        (blocks + ROWS - height, LANES), jnp.float32
                    )
                else:
                    total[b, parity, half, 0:height, :] += high[:, lanes] + low[:, lanes]

    build(0, 0, even)
    pieces = LANES // per_batch
    taps = [
        jnp.concatenate(
            [rows_of(half * pieces + piece, SENT - 1)[:, :per_batch] for piece in range(pieces)],
            axis=1,
        )
        for half in range(HALVES)
    ]
    high = [half.astype(jnp.bfloat16).astype(jnp.float32) for half in taps]
    put_in_order(batch, high)
    put_in_order(batch + 1, [half - part for half, part in zip(taps, high)])
    for b in range(batch):
        put_in_order(b, [rows_of(b, half) for half in range(HALVES)])
    total[batch] = jnp.zeros(total.shape[1:], jnp.float32)

    def one_batch(b, last):
        for group in range(groups):
            now, later = (even, odd) if group % 2 == 0 else (odd, even)
            if group + 1 < groups:
                build(b, group + 1, later)
            elif not last:
                build(b + 1, 0, later)
            multiply(b, group, now)

    def one_step(b, carry):
        one_batch(b, False)
        return carry

    lax.fori_loop(0, batch - 1, one_step, 0)
    one_batch(batch - 1, True)

    last_lane = lax.broadcasted_iota(jnp.int32, (blocks, LANES), 1) == LANES - 1
    for kind in range(batch + 1):
        late = [pltpu.roll(total[kind, 1, half, 0:blocks, :], LANES - 1, 1) for half in range(HALVES)]
        late.append(pltpu.roll(total[kind, 1, 0, 1 : blocks + 1, :], LANES - 1, 1))
        for half in range(HALVES):
            joined = total[kind, 0, half, 0:blocks, :] + jnp.where(
                last_lane, late[half + 1], late[half]
            )
            if kind < batch:
                joined = joined + gain * rows_of(kind, HALVES + half)
                out_ref[pl.ds(kind * blocks * BACK + half, blocks, stride=BACK), :] = joined
            else:
                for b in range(half, batch, HALVES):
                    out_ref[pl.ds(b * blocks * BACK + HALVES, blocks, stride=BACK), :] = joined


def correlations(got, batch, blocks):
    hankel = pltpu.VMEM(((2 * PACK + 3) * LANES // 2, LANES), jnp.bfloat16)
    return pl.pallas_call(
        functools.partial(correlate, batch, blocks),
        out_shape=jax.ShapeDtypeStruct((batch * blocks * BACK, LANES), jnp.float32),
        in_specs=[pl.BlockSpec(memory_space=pltpu.VMEM)],
        out_specs=pl.BlockSpec(memory_space=pltpu.VMEM),
        scratch_shapes=[
            hankel,
            hankel,
            pltpu.VMEM((batch + 2, 2, blocks + PACK, LANES), jnp.float32),
            pltpu.VMEM((batch + 1, 2, HALVES, blocks + ROWS, LANES), jnp.float32),
        ],
        compiler_params=pltpu.CompilerParams(vmem_limit_bytes=24 * 1024 * 1024),
        cost_estimate=pl.CostEstimate(flops=6_000_000_000, bytes_accessed=2_000_000, transcendentals=0),
        name="correlate",
    )(got)


def write_out(pairs, left):
    copies = [
        pltpu.make_async_copy(source, target, left.at[place])
        for place, (source, target) in enumerate(pairs)
    ]
    for copy in copies:
        copy.start()
    return copies


def turn(home_ref, half_ref):
    channels = half_ref.shape[1]
    half_ref[...] = home_ref[pl.ds(HALVES, channels, stride=BACK), :].T


def filter_half(home):
    channels = home.shape[0] // BACK
    vmem = pl.BlockSpec(memory_space=pltpu.VMEM)
    return pl.pallas_call(
        turn,
        out_shape=jax.ShapeDtypeStruct((LANES, channels), jnp.float32),
        in_specs=[vmem],
        out_specs=vmem,
        compiler_params=pltpu.CompilerParams(vmem_limit_bytes=16 * 1024 * 1024),
        name="turn",
    )(home)


def finish(home_ref, input_ref, own, left):
    channels = input_ref.shape[2]
    copies = []
    for half in range(HALVES):
        rows = slice(half * LANES, (half + 1) * LANES)
        conv = home_ref[pl.ds(half, channels, stride=BACK), :].T
        own[0, rows, :] = conv.astype(jnp.bfloat16)
        copies += write_out([(own.at[:, rows, :], input_ref.at[:, rows, :])], left.at[pl.ds(half, 1)])
    for copy in copies:
        copy.wait()


def input_gradient(home):
    channels = home.shape[0] // BACK
    return pl.pallas_call(
        finish,
        out_shape=jax.ShapeDtypeStruct((1, BLOCK, channels), jnp.bfloat16),
        in_specs=[pl.BlockSpec(memory_space=pltpu.VMEM)],
        out_specs=pl.BlockSpec(memory_space=pltpu.HBM),
        scratch_shapes=[
            pltpu.VMEM((1, BLOCK, channels), jnp.bfloat16),
            pltpu.SemaphoreType.DMA((HALVES,)),
        ],
        compiler_params=pltpu.CompilerParams(vmem_limit_bytes=16 * 1024 * 1024),
        cost_estimate=pl.CostEstimate(flops=1_000_000_000, bytes_accessed=1_000_000, transcendentals=0),
        name="finish",
    )(home)


def join(own_ref, other_ref, filter_ref, left):
    core = lax.rem(lax.axis_index("batch"), HALVES)
    copies = write_out(
        [
            (own_ref, filter_ref.at[pl.ds(pl.multiple_of(core * LANES, LANES), LANES), :]),
            (other_ref, filter_ref.at[pl.ds(pl.multiple_of((1 - core) * LANES, LANES), LANES), :]),
        ],
        left,
    )
    for copy in copies:
        copy.wait()


def filter_gradient(own, other):
    vmem = pl.BlockSpec(memory_space=pltpu.VMEM)
    return pl.pallas_call(
        join,
        out_shape=jax.ShapeDtypeStruct((BLOCK, own.shape[1]), jnp.float32),
        in_specs=[vmem, vmem],
        out_specs=pl.BlockSpec(memory_space=pltpu.HBM),
        scratch_shapes=[pltpu.SemaphoreType.DMA((HALVES,))],
        compiler_params=pltpu.CompilerParams(vmem_limit_bytes=16 * 1024 * 1024),
        name="join",
    )(own, other)


def shards(signal, grad_out, filter_taps, skip_gain):
    batch, blocks = lax.axis_size("batch"), lax.axis_size("seq")
    axes = ("batch", "seq")
    channels = filter_taps.shape[1]
    grad_rows = grad_out[0].astype(jnp.float32)
    signal_rows = signal[0].astype(jnp.float32)
    per_batch = BLOCK // batch
    gain = jnp.broadcast_to(skip_gain[None, :], (LANES - per_batch, channels))
    signal_rows, grad_rows, gain = lax.optimization_barrier((signal_rows, grad_rows, gain))
    sent = pieces_to_send(signal_rows, grad_rows, filter_taps, gain, per_batch)
    sent = sent.reshape(channels, SENT, 1, LANES)
    got = lax.all_to_all(sent, axes, 0, 0, tiled=True)
    back = correlations(got.reshape(channels * SENT, LANES), batch, blocks)
    home = lax.all_to_all(back.reshape(channels, BACK, 1, LANES), axes, 0, 0, tiled=True)
    home = home.reshape(channels * BACK, LANES)
    own = filter_half(home)
    other = lax.ppermute(own, "batch", [(b, b ^ 1) for b in range(batch)])
    return (input_gradient(home), filter_gradient(own, other))


def solution(mesh):
    return jax.shard_map(
        shards,
        mesh=mesh,
        in_specs=(P("batch", "seq", None), P("batch", "seq", None), P("seq", None), P()),
        out_specs=(P("batch", "seq", None), P("seq", None)),
        check_vma=False,
    )
```

```python
import functools

import jax
import jax.numpy as jnp
from jax import lax
from jax.experimental import pallas as pl
from jax.experimental.pallas import tpu as pltpu
from jax.sharding import PartitionSpec as P

LANES = 128
ROWS = 8
BLOCK = 256
HALVES = BLOCK // LANES
PACK = 16
SENT = 5
BACK = 3


def product(left, right):
    return jnp.dot(left, right, preferred_element_type=jnp.float32)


def send(per_batch, signal_ref, grad_ref, taps_ref, gain_ref, sent_ref):
    channels = gain_ref.shape[1]
    for half in range(HALVES):
        rows = slice(half * LANES, (half + 1) * LANES)
        sent_ref[pl.ds(half, channels, stride=SENT), :] = signal_ref[rows, :].T
        sent_ref[pl.ds(HALVES + half, channels, stride=SENT), :] = grad_ref[rows, :].T
    first = pl.multiple_of(lax.axis_index("batch") * per_batch, per_batch)
    taps = taps_ref[pl.ds(first, per_batch), :]
    sent_ref[pl.ds(SENT - 1, channels, stride=SENT), :] = jnp.concatenate(
        [taps, gain_ref[...]], axis=0
    ).T


def pieces_to_send(signal_rows, grad_rows, filter_taps, gain, per_batch):
    channels = gain.shape[1]
    vmem = pl.BlockSpec(memory_space=pltpu.VMEM)
    return pl.pallas_call(
        functools.partial(send, per_batch),
        out_shape=jax.ShapeDtypeStruct((channels * SENT, LANES), jnp.float32),
        in_specs=[vmem] * 4,
        out_specs=vmem,
        compiler_params=pltpu.CompilerParams(vmem_limit_bytes=16 * 1024 * 1024),
        name="send",
    )(signal_rows, grad_rows, filter_taps, gain)


def correlate(batch, blocks, got_ref, out_ref, even, odd, ordered, total):
    groups = blocks // PACK
    per_batch = BLOCK // batch
    window = LANES // 2
    gain = jnp.broadcast_to(got_ref[SENT - 1 : SENT, per_batch : per_batch + 1], (1, LANES))
    row = lax.broadcasted_iota(jnp.int32, (window, LANES), 0)
    lane = lax.broadcasted_iota(jnp.int32, (window, LANES), 1)
    own = lane <= 2 * row + 1
    nothing = jnp.zeros((window, LANES), jnp.float32)
    source = lax.broadcasted_iota(jnp.int32, (BLOCK, BLOCK), 0)
    target = lax.broadcasted_iota(jnp.int32, (BLOCK, BLOCK), 1)
    step = source // 2
    place = LANES * (source % 2) + window * (step // window) + (window - 1 - step % window)
    lanes_to = jnp.where(place == target, 1.0, 0.0).astype(jnp.bfloat16)
    target = lax.broadcasted_iota(jnp.int32, (blocks, blocks), 0)
    source = lax.broadcasted_iota(jnp.int32, (blocks, blocks), 1)
    rows_to = jnp.where(source + target == blocks - 1, 1.0, 0.0).astype(jnp.bfloat16)

    def rows_of(b, part):
        return got_ref[pl.ds(b * blocks * SENT + part, blocks, stride=SENT), :]

    def put_in_order(kind, halves):
        values = jnp.concatenate(halves, axis=1).astype(jnp.bfloat16)
        moved = product(rows_to, product(values, lanes_to).astype(jnp.bfloat16))
        for parity in range(2):
            ordered[kind, parity, 0:blocks, :] = moved[:, parity * LANES : (parity + 1) * LANES]
            ordered[kind, parity, blocks : blocks + PACK, :] = jnp.zeros((PACK, LANES), jnp.float32)

    def turned(b, block):
        values = got_ref[pl.ds((b * blocks + block // 2) * SENT + HALVES + block % 2, 1), :]
        return pltpu.roll(jnp.broadcast_to(values, (window, LANES)), 2, 1, stride=2, stride_axis=0)

    def build(b, group, hankel):
        first = 2 * PACK * group

        def at(block):
            return turned(b, block) if block < 2 * blocks else nothing

        current = at(first)
        for inner in range(2 * PACK + 3):
            following = at(first + inner + 1)
            hankel[inner * window : (inner + 1) * window, :] = jnp.where(
                own, current, following
            ).astype(jnp.bfloat16)
            current = following

    def multiply(b, group, part, hankel):
        height = PACK * group + ROWS * (part + 1)
        result = None
        for inner in range(part * ROWS // 2, (part + 1) * ROWS // 2):
            start = blocks - 1 - PACK * group - 2 * inner
            left = jnp.concatenate(
                [
                    jnp.concatenate(
                        [
                            ordered[kind, parity, pl.ds(start - later, height), :]
                            for later in range(2)
                        ],
                        axis=1,
                    )
                    for kind in (b, batch, batch + 1)
                    for parity in range(2)
                ],
                axis=0,
            ).astype(jnp.bfloat16)
            right = jnp.concatenate(
                [
                    hankel[(4 * inner + half) * window : (4 * inner + half) * window + BLOCK, :]
                    for half in range(HALVES)
                ],
                axis=1,
            )
            term = product(left, right)
            result = term if result is None else result + term
        for parity in range(2):
            shared = result[parity * height : (parity + 1) * height]
            high = result[(2 + parity) * height : (3 + parity) * height]
            low = result[(4 + parity) * height : (5 + parity) * height]
            for half in range(HALVES):
                lanes = slice(half * LANES, (half + 1) * LANES)
                total[batch, parity, half, 0:height, :] += shared[:, lanes]
                if group == 0 and part == 0:
                    total[b, parity, half, 0:height, :] = high[:, lanes] + low[:, lanes]
                    total[b, parity, half, height : blocks + ROWS, :] = jnp.zeros(
                        (blocks + ROWS - height, LANES), jnp.float32
                    )
                else:
                    total[b, parity, half, 0:height, :] += high[:, lanes] + low[:, lanes]

    build(0, 0, even)
    pieces = LANES // per_batch
    taps = [
        jnp.concatenate(
            [rows_of(half * pieces + piece, SENT - 1)[:, :per_batch] for piece in range(pieces)],
            axis=1,
        )
        for half in range(HALVES)
    ]
    high = [half.astype(jnp.bfloat16).astype(jnp.float32) for half in taps]
    put_in_order(batch, high)
    put_in_order(batch + 1, [half - part for half, part in zip(taps, high)])
    for b in range(batch):
        put_in_order(b, [rows_of(b, half) for half in range(HALVES)])
    total[batch] = jnp.zeros(total.shape[1:], jnp.float32)

    def one_batch(b, last):
        for group in range(groups):
            now, later = (even, odd) if group % 2 == 0 else (odd, even)
            if group + 1 < groups:
                build(b, group + 1, later)
            elif not last:
                build(b + 1, 0, later)
            for part in range(PACK // ROWS):
                multiply(b, group, part, now)

    def one_step(b, carry):
        one_batch(b, False)
        return carry

    lax.fori_loop(0, batch - 1, one_step, 0)
    one_batch(batch - 1, True)

    last_lane = lax.broadcasted_iota(jnp.int32, (blocks, LANES), 1) == LANES - 1
    for kind in range(batch + 1):
        late = [pltpu.roll(total[kind, 1, half, 0:blocks, :], LANES - 1, 1) for half in range(HALVES)]
        late.append(pltpu.roll(total[kind, 1, 0, 1 : blocks + 1, :], LANES - 1, 1))
        for half in range(HALVES):
            joined = total[kind, 0, half, 0:blocks, :] + jnp.where(
                last_lane, late[half + 1], late[half]
            )
            if kind < batch:
                joined = joined + gain * rows_of(kind, HALVES + half)
                out_ref[pl.ds(kind * blocks * BACK + half, blocks, stride=BACK), :] = joined
            else:
                for b in range(half, batch, HALVES):
                    out_ref[pl.ds(b * blocks * BACK + HALVES, blocks, stride=BACK), :] = joined


def correlations(got, batch, blocks):
    hankel = pltpu.VMEM(((2 * PACK + 3) * LANES // 2, LANES), jnp.bfloat16)
    return pl.pallas_call(
        functools.partial(correlate, batch, blocks),
        out_shape=jax.ShapeDtypeStruct((batch * blocks * BACK, LANES), jnp.float32),
        in_specs=[pl.BlockSpec(memory_space=pltpu.VMEM)],
        out_specs=pl.BlockSpec(memory_space=pltpu.VMEM),
        scratch_shapes=[
            hankel,
            hankel,
            pltpu.VMEM((batch + 2, 2, blocks + PACK, LANES), jnp.float32),
            pltpu.VMEM((batch + 1, 2, HALVES, blocks + ROWS, LANES), jnp.float32),
        ],
        compiler_params=pltpu.CompilerParams(vmem_limit_bytes=24 * 1024 * 1024),
        cost_estimate=pl.CostEstimate(flops=6_000_000_000, bytes_accessed=2_000_000, transcendentals=0),
        name="correlate",
    )(got)


def write_out(pairs, left):
    copies = [
        pltpu.make_async_copy(source, target, left.at[place])
        for place, (source, target) in enumerate(pairs)
    ]
    for copy in copies:
        copy.start()
    return copies


def turn(home_ref, half_ref):
    channels = half_ref.shape[1]
    half_ref[...] = home_ref[pl.ds(HALVES, channels, stride=BACK), :].T


def filter_half(home):
    channels = home.shape[0] // BACK
    vmem = pl.BlockSpec(memory_space=pltpu.VMEM)
    return pl.pallas_call(
        turn,
        out_shape=jax.ShapeDtypeStruct((LANES, channels), jnp.float32),
        in_specs=[vmem],
        out_specs=vmem,
        compiler_params=pltpu.CompilerParams(vmem_limit_bytes=16 * 1024 * 1024),
        name="turn",
    )(home)


def finish(home_ref, input_ref, own, left):
    channels = input_ref.shape[2]
    copies = []
    for half in range(HALVES):
        rows = slice(half * LANES, (half + 1) * LANES)
        conv = home_ref[pl.ds(half, channels, stride=BACK), :].T
        own[0, rows, :] = conv.astype(jnp.bfloat16)
        copies += write_out([(own.at[:, rows, :], input_ref.at[:, rows, :])], left.at[pl.ds(half, 1)])
    for copy in copies:
        copy.wait()


def input_gradient(home):
    channels = home.shape[0] // BACK
    return pl.pallas_call(
        finish,
        out_shape=jax.ShapeDtypeStruct((1, BLOCK, channels), jnp.bfloat16),
        in_specs=[pl.BlockSpec(memory_space=pltpu.VMEM)],
        out_specs=pl.BlockSpec(memory_space=pltpu.HBM),
        scratch_shapes=[
            pltpu.VMEM((1, BLOCK, channels), jnp.bfloat16),
            pltpu.SemaphoreType.DMA((HALVES,)),
        ],
        compiler_params=pltpu.CompilerParams(vmem_limit_bytes=16 * 1024 * 1024),
        cost_estimate=pl.CostEstimate(flops=1_000_000_000, bytes_accessed=1_000_000, transcendentals=0),
        name="finish",
    )(home)


def join(own_ref, other_ref, filter_ref, left):
    core = lax.rem(lax.axis_index("batch"), HALVES)
    copies = write_out(
        [
            (own_ref, filter_ref.at[pl.ds(pl.multiple_of(core * LANES, LANES), LANES), :]),
            (other_ref, filter_ref.at[pl.ds(pl.multiple_of((1 - core) * LANES, LANES), LANES), :]),
        ],
        left,
    )
    for copy in copies:
        copy.wait()


def filter_gradient(own, other):
    vmem = pl.BlockSpec(memory_space=pltpu.VMEM)
    return pl.pallas_call(
        join,
        out_shape=jax.ShapeDtypeStruct((BLOCK, own.shape[1]), jnp.float32),
        in_specs=[vmem, vmem],
        out_specs=pl.BlockSpec(memory_space=pltpu.HBM),
        scratch_shapes=[pltpu.SemaphoreType.DMA((HALVES,))],
        compiler_params=pltpu.CompilerParams(vmem_limit_bytes=16 * 1024 * 1024),
        name="join",
    )(own, other)


def shards(signal, grad_out, filter_taps, skip_gain):
    batch, blocks = lax.axis_size("batch"), lax.axis_size("seq")
    axes = ("batch", "seq")
    channels = filter_taps.shape[1]
    grad_rows = grad_out[0].astype(jnp.float32)
    signal_rows = signal[0].astype(jnp.float32)
    per_batch = BLOCK // batch
    gain = jnp.broadcast_to(skip_gain[None, :], (LANES - per_batch, channels))
    signal_rows, grad_rows, gain = lax.optimization_barrier((signal_rows, grad_rows, gain))
    sent = pieces_to_send(signal_rows, grad_rows, filter_taps, gain, per_batch)
    sent = sent.reshape(channels, SENT, 1, LANES)
    got = lax.all_to_all(sent, axes, 0, 0, tiled=True)
    back = correlations(got.reshape(channels * SENT, LANES), batch, blocks)
    home = lax.all_to_all(back.reshape(channels, BACK, 1, LANES), axes, 0, 0, tiled=True)
    home = home.reshape(channels * BACK, LANES)
    own = filter_half(home)
    other = lax.ppermute(own, "batch", [(b, b ^ 1) for b in range(batch)])
    return (input_gradient(home), filter_gradient(own, other))


def solution(mesh):
    return jax.shard_map(
        shards,
        mesh=mesh,
        in_specs=(P("batch", "seq", None), P("batch", "seq", None), P("seq", None), P()),
        out_specs=(P("batch", "seq", None), P("seq", None)),
        check_vma=False,
    )
```

```python
import functools

import jax
import jax.numpy as jnp
from jax import lax
from jax.experimental import pallas as pl
from jax.experimental.pallas import tpu as pltpu
from jax.sharding import PartitionSpec as P

LANES = 128
ROWS = 8
BLOCK = 256
HALVES = BLOCK // LANES
PACK = 16
SENT = 5
BACK = 3


def product(left, right):
    return jnp.dot(left, right, preferred_element_type=jnp.float32)


def send(per_batch, signal_ref, grad_ref, taps_ref, gain_ref, sent_ref):
    channels = gain_ref.shape[1]
    for half in range(HALVES):
        rows = slice(half * LANES, (half + 1) * LANES)
        sent_ref[pl.ds(half, channels, stride=SENT), :] = signal_ref[rows, :].T
        sent_ref[pl.ds(HALVES + half, channels, stride=SENT), :] = grad_ref[rows, :].T
    first = pl.multiple_of(lax.axis_index("batch") * per_batch, per_batch)
    taps = taps_ref[pl.ds(first, per_batch), :]
    sent_ref[pl.ds(SENT - 1, channels, stride=SENT), :] = jnp.concatenate(
        [taps, gain_ref[...]], axis=0
    ).T


def pieces_to_send(signal_rows, grad_rows, filter_taps, gain, per_batch):
    channels = gain.shape[1]
    vmem = pl.BlockSpec(memory_space=pltpu.VMEM)
    return pl.pallas_call(
        functools.partial(send, per_batch),
        out_shape=jax.ShapeDtypeStruct((channels * SENT, LANES), jnp.float32),
        in_specs=[vmem] * 4,
        out_specs=vmem,
        compiler_params=pltpu.CompilerParams(vmem_limit_bytes=16 * 1024 * 1024),
        name="send",
    )(signal_rows, grad_rows, filter_taps, gain)


def correlate(batch, blocks, got_ref, out_ref, even, odd, ordered, total):
    groups = blocks // PACK
    per_batch = BLOCK // batch
    window = LANES // 2
    gain = jnp.broadcast_to(got_ref[SENT - 1 : SENT, per_batch : per_batch + 1], (1, LANES))
    row = lax.broadcasted_iota(jnp.int32, (window, LANES), 0)
    lane = lax.broadcasted_iota(jnp.int32, (window, LANES), 1)
    own = lane <= 2 * row + 1
    nothing = jnp.zeros((window, LANES), jnp.float32)
    source = lax.broadcasted_iota(jnp.int32, (BLOCK, BLOCK), 0)
    target = lax.broadcasted_iota(jnp.int32, (BLOCK, BLOCK), 1)
    step = source // 2
    place = LANES * (source % 2) + window * (step // window) + (window - 1 - step % window)
    lanes_to = jnp.where(place == target, 1.0, 0.0).astype(jnp.bfloat16)
    target = lax.broadcasted_iota(jnp.int32, (blocks, blocks), 0)
    source = lax.broadcasted_iota(jnp.int32, (blocks, blocks), 1)
    rows_to = jnp.where(source + target == blocks - 1, 1.0, 0.0).astype(jnp.bfloat16)

    def rows_of(b, part):
        return got_ref[pl.ds(b * blocks * SENT + part, blocks, stride=SENT), :]

    def put_in_order(kind, halves):
        values = jnp.concatenate(halves, axis=1).astype(jnp.bfloat16)
        moved = product(rows_to, product(values, lanes_to).astype(jnp.bfloat16))
        for parity in range(2):
            ordered[kind, parity, 0:blocks, :] = moved[:, parity * LANES : (parity + 1) * LANES]
            ordered[kind, parity, blocks : blocks + PACK, :] = jnp.zeros((PACK, LANES), jnp.float32)

    def turned(b, block):
        values = got_ref[pl.ds((b * blocks + block // 2) * SENT + HALVES + block % 2, 1), :]
        return pltpu.roll(jnp.broadcast_to(values, (window, LANES)), 2, 1, stride=2, stride_axis=0)

    def build(b, group, hankel):
        first = 2 * PACK * group

        def at(block):
            return turned(b, block) if block < 2 * blocks else nothing

        current = at(first)
        for inner in range(2 * PACK + 3):
            following = at(first + inner + 1)
            hankel[inner * window : (inner + 1) * window, :] = jnp.where(
                own, current, following
            ).astype(jnp.bfloat16)
            current = following

    def multiply(b, group, part, hankel):
        height = PACK * group + ROWS * (part + 1)
        result = None
        for inner in range(part * ROWS // 2, (part + 1) * ROWS // 2):
            start = blocks - 1 - PACK * group - 2 * inner
            left = jnp.concatenate(
                [
                    jnp.concatenate(
                        [
                            ordered[kind, parity, pl.ds(start - later, height), :]
                            for later in range(2)
                        ],
                        axis=1,
                    )
                    for kind in (b, batch, batch + 1)
                    for parity in range(2)
                ],
                axis=0,
            ).astype(jnp.bfloat16)
            right = jnp.concatenate(
                [
                    hankel[(4 * inner + half) * window : (4 * inner + half) * window + BLOCK, :]
                    for half in range(HALVES)
                ],
                axis=1,
            )
            term = product(left, right)
            result = term if result is None else result + term
        for parity in range(2):
            shared = result[parity * height : (parity + 1) * height]
            high = result[(2 + parity) * height : (3 + parity) * height]
            low = result[(4 + parity) * height : (5 + parity) * height]
            for half in range(HALVES):
                lanes = slice(half * LANES, (half + 1) * LANES)
                total[batch, parity, half, 0:height, :] += shared[:, lanes]
                if group == 0 and part == 0:
                    total[b, parity, half, 0:height, :] = high[:, lanes] + low[:, lanes]
                    total[b, parity, half, height : blocks + ROWS, :] = jnp.zeros(
                        (blocks + ROWS - height, LANES), jnp.float32
                    )
                else:
                    total[b, parity, half, 0:height, :] += high[:, lanes] + low[:, lanes]

    build(0, 0, even)
    pieces = LANES // per_batch
    taps = [
        jnp.concatenate(
            [rows_of(half * pieces + piece, SENT - 1)[:, :per_batch] for piece in range(pieces)],
            axis=1,
        )
        for half in range(HALVES)
    ]
    high = [half.astype(jnp.bfloat16).astype(jnp.float32) for half in taps]
    put_in_order(batch, high)
    put_in_order(batch + 1, [half - part for half, part in zip(taps, high)])
    for b in range(batch):
        put_in_order(b, [rows_of(b, half) for half in range(HALVES)])
    total[batch] = jnp.zeros(total.shape[1:], jnp.float32)

    def one_batch(b, last):
        for group in range(groups):
            now, later = (even, odd) if group % 2 == 0 else (odd, even)
            if group + 1 < groups:
                build(b, group + 1, later)
            elif not last:
                build(b + 1, 0, later)
            for part in range(PACK // ROWS):
                multiply(b, group, part, now)

    for b in range(batch):
        one_batch(b, b == batch - 1)

    last_lane = lax.broadcasted_iota(jnp.int32, (blocks, LANES), 1) == LANES - 1
    for kind in range(batch + 1):
        late = [pltpu.roll(total[kind, 1, half, 0:blocks, :], LANES - 1, 1) for half in range(HALVES)]
        late.append(pltpu.roll(total[kind, 1, 0, 1 : blocks + 1, :], LANES - 1, 1))
        for half in range(HALVES):
            joined = total[kind, 0, half, 0:blocks, :] + jnp.where(
                last_lane, late[half + 1], late[half]
            )
            if kind < batch:
                joined = joined + gain * rows_of(kind, HALVES + half)
                out_ref[pl.ds(kind * blocks * BACK + half, blocks, stride=BACK), :] = joined
            else:
                for b in range(half, batch, HALVES):
                    out_ref[pl.ds(b * blocks * BACK + HALVES, blocks, stride=BACK), :] = joined


def correlations(got, batch, blocks):
    hankel = pltpu.VMEM(((2 * PACK + 3) * LANES // 2, LANES), jnp.bfloat16)
    return pl.pallas_call(
        functools.partial(correlate, batch, blocks),
        out_shape=jax.ShapeDtypeStruct((batch * blocks * BACK, LANES), jnp.float32),
        in_specs=[pl.BlockSpec(memory_space=pltpu.VMEM)],
        out_specs=pl.BlockSpec(memory_space=pltpu.VMEM),
        scratch_shapes=[
            hankel,
            hankel,
            pltpu.VMEM((batch + 2, 2, blocks + PACK, LANES), jnp.float32),
            pltpu.VMEM((batch + 1, 2, HALVES, blocks + ROWS, LANES), jnp.float32),
        ],
        compiler_params=pltpu.CompilerParams(vmem_limit_bytes=24 * 1024 * 1024),
        cost_estimate=pl.CostEstimate(flops=6_000_000_000, bytes_accessed=2_000_000, transcendentals=0),
        name="correlate",
    )(got)


def write_out(pairs, left):
    copies = [
        pltpu.make_async_copy(source, target, left.at[place])
        for place, (source, target) in enumerate(pairs)
    ]
    for copy in copies:
        copy.start()
    return copies


def turn(home_ref, half_ref):
    channels = half_ref.shape[1]
    half_ref[...] = home_ref[pl.ds(HALVES, channels, stride=BACK), :].T


def filter_half(home):
    channels = home.shape[0] // BACK
    vmem = pl.BlockSpec(memory_space=pltpu.VMEM)
    return pl.pallas_call(
        turn,
        out_shape=jax.ShapeDtypeStruct((LANES, channels), jnp.float32),
        in_specs=[vmem],
        out_specs=vmem,
        compiler_params=pltpu.CompilerParams(vmem_limit_bytes=16 * 1024 * 1024),
        name="turn",
    )(home)


def finish(home_ref, input_ref, own, left):
    channels = input_ref.shape[2]
    copies = []
    for half in range(HALVES):
        rows = slice(half * LANES, (half + 1) * LANES)
        conv = home_ref[pl.ds(half, channels, stride=BACK), :].T
        own[0, rows, :] = conv.astype(jnp.bfloat16)
        copies += write_out([(own.at[:, rows, :], input_ref.at[:, rows, :])], left.at[pl.ds(half, 1)])
    for copy in copies:
        copy.wait()


def input_gradient(home):
    channels = home.shape[0] // BACK
    return pl.pallas_call(
        finish,
        out_shape=jax.ShapeDtypeStruct((1, BLOCK, channels), jnp.bfloat16),
        in_specs=[pl.BlockSpec(memory_space=pltpu.VMEM)],
        out_specs=pl.BlockSpec(memory_space=pltpu.HBM),
        scratch_shapes=[
            pltpu.VMEM((1, BLOCK, channels), jnp.bfloat16),
            pltpu.SemaphoreType.DMA((HALVES,)),
        ],
        compiler_params=pltpu.CompilerParams(vmem_limit_bytes=16 * 1024 * 1024),
        cost_estimate=pl.CostEstimate(flops=1_000_000_000, bytes_accessed=1_000_000, transcendentals=0),
        name="finish",
    )(home)


def join(own_ref, other_ref, filter_ref, left):
    core = lax.rem(lax.axis_index("batch"), HALVES)
    copies = write_out(
        [
            (own_ref, filter_ref.at[pl.ds(pl.multiple_of(core * LANES, LANES), LANES), :]),
            (other_ref, filter_ref.at[pl.ds(pl.multiple_of((1 - core) * LANES, LANES), LANES), :]),
        ],
        left,
    )
    for copy in copies:
        copy.wait()


def filter_gradient(own, other):
    vmem = pl.BlockSpec(memory_space=pltpu.VMEM)
    return pl.pallas_call(
        join,
        out_shape=jax.ShapeDtypeStruct((BLOCK, own.shape[1]), jnp.float32),
        in_specs=[vmem, vmem],
        out_specs=pl.BlockSpec(memory_space=pltpu.HBM),
        scratch_shapes=[pltpu.SemaphoreType.DMA((HALVES,))],
        compiler_params=pltpu.CompilerParams(vmem_limit_bytes=16 * 1024 * 1024),
        name="join",
    )(own, other)


def shards(signal, grad_out, filter_taps, skip_gain):
    batch, blocks = lax.axis_size("batch"), lax.axis_size("seq")
    axes = ("batch", "seq")
    channels = filter_taps.shape[1]
    grad_rows = grad_out[0].astype(jnp.float32)
    signal_rows = signal[0].astype(jnp.float32)
    per_batch = BLOCK // batch
    gain = jnp.broadcast_to(skip_gain[None, :], (LANES - per_batch, channels))
    signal_rows, grad_rows, gain = lax.optimization_barrier((signal_rows, grad_rows, gain))
    sent = pieces_to_send(signal_rows, grad_rows, filter_taps, gain, per_batch)
    sent = sent.reshape(channels, SENT, 1, LANES)
    got = lax.all_to_all(sent, axes, 0, 0, tiled=True)
    back = correlations(got.reshape(channels * SENT, LANES), batch, blocks)
    home = lax.all_to_all(back.reshape(channels, BACK, 1, LANES), axes, 0, 0, tiled=True)
    home = home.reshape(channels * BACK, LANES)
    own = filter_half(home)
    other = lax.ppermute(own, "batch", [(b, b ^ 1) for b in range(batch)])
    return (input_gradient(home), filter_gradient(own, other))


def solution(mesh):
    return jax.shard_map(
        shards,
        mesh=mesh,
        in_specs=(P("batch", "seq", None), P("batch", "seq", None), P("seq", None), P()),
        out_specs=(P("batch", "seq", None), P("seq", None)),
        check_vma=False,
    )
```

```python
import functools

import jax
import jax.numpy as jnp
from jax import lax
from jax.experimental import pallas as pl
from jax.experimental.pallas import tpu as pltpu
from jax.sharding import PartitionSpec as P

LANES = 128
ROWS = 8
BLOCK = 256
HALVES = BLOCK // LANES
PACK = 16
SENT = 5
BACK = 3


def product(left, right):
    return jnp.dot(left, right, preferred_element_type=jnp.float32)


def send(per_batch, signal_ref, grad_ref, taps_ref, gain_ref, sent_ref):
    channels = gain_ref.shape[1]
    for half in range(HALVES):
        rows = slice(half * LANES, (half + 1) * LANES)
        sent_ref[pl.ds(half, channels, stride=SENT), :] = signal_ref[rows, :].T
        sent_ref[pl.ds(HALVES + half, channels, stride=SENT), :] = grad_ref[rows, :].T
    b = lax.axis_index("batch")
    taps = taps_ref[pl.ds(pl.multiple_of(b * per_batch, per_batch), per_batch), :]
    row = lax.broadcasted_iota(jnp.int32, (LANES, channels), 0)
    last = jnp.where(
        row // per_batch == lax.rem(b, LANES // per_batch),
        jnp.concatenate([taps, taps], axis=0),
        jnp.concatenate([gain_ref[...], gain_ref[...]], axis=0),
    )
    sent_ref[pl.ds(SENT - 1, channels, stride=SENT), :] = last.T


def pieces_to_send(signal_rows, grad_rows, filter_taps, gain, per_batch):
    channels = gain.shape[1]
    vmem = pl.BlockSpec(memory_space=pltpu.VMEM)
    return pl.pallas_call(
        functools.partial(send, per_batch),
        out_shape=jax.ShapeDtypeStruct((channels * SENT, LANES), jnp.float32),
        in_specs=[vmem] * 4,
        out_specs=vmem,
        compiler_params=pltpu.CompilerParams(vmem_limit_bytes=16 * 1024 * 1024),
        name="send",
    )(signal_rows, grad_rows, filter_taps, gain)


def correlate(batch, blocks, got_ref, out_ref, even, odd, ordered, total):
    groups = blocks // PACK
    per_batch = BLOCK // batch
    window = LANES // 2
    gain = jnp.broadcast_to(got_ref[SENT - 1 : SENT, per_batch : per_batch + 1], (1, LANES))
    row = lax.broadcasted_iota(jnp.int32, (window, LANES), 0)
    lane = lax.broadcasted_iota(jnp.int32, (window, LANES), 1)
    own = lane <= 2 * row + 1
    nothing = jnp.zeros((window, LANES), jnp.float32)
    source = lax.broadcasted_iota(jnp.int32, (BLOCK, BLOCK), 0)
    target = lax.broadcasted_iota(jnp.int32, (BLOCK, BLOCK), 1)
    step = source // 2
    place = LANES * (source % 2) + window * (step // window) + (window - 1 - step % window)
    lanes_to = jnp.where(place == target, 1.0, 0.0).astype(jnp.bfloat16)
    target = lax.broadcasted_iota(jnp.int32, (blocks, blocks), 0)
    source = lax.broadcasted_iota(jnp.int32, (blocks, blocks), 1)
    rows_to = jnp.where(source + target == blocks - 1, 1.0, 0.0).astype(jnp.bfloat16)

    def rows_of(b, part):
        return got_ref[pl.ds(b * blocks * SENT + part, blocks, stride=SENT), :]

    def put_in_order(kind, halves):
        values = jnp.concatenate(halves, axis=1).astype(jnp.bfloat16)
        moved = product(rows_to, product(values, lanes_to).astype(jnp.bfloat16))
        for parity in range(2):
            ordered[kind, parity, 0:blocks, :] = moved[:, parity * LANES : (parity + 1) * LANES]
            ordered[kind, parity, blocks : blocks + PACK, :] = jnp.zeros((PACK, LANES), jnp.float32)

    def turned(b, block):
        values = got_ref[pl.ds((b * blocks + block // 2) * SENT + HALVES + block % 2, 1), :]
        return pltpu.roll(jnp.broadcast_to(values, (window, LANES)), 2, 1, stride=2, stride_axis=0)

    def build(b, group, hankel):
        first = 2 * PACK * group

        def at(block):
            return turned(b, block) if block < 2 * blocks else nothing

        current = at(first)
        for inner in range(2 * PACK + 3):
            following = at(first + inner + 1)
            hankel[inner * window : (inner + 1) * window, :] = jnp.where(
                own, current, following
            ).astype(jnp.bfloat16)
            current = following

    def multiply(b, group, part, hankel):
        height = PACK * group + ROWS * (part + 1)
        result = None
        for inner in range(part * ROWS // 2, (part + 1) * ROWS // 2):
            start = blocks - 1 - PACK * group - 2 * inner
            left = jnp.concatenate(
                [
                    jnp.concatenate(
                        [
                            ordered[kind, parity, pl.ds(start - later, height), :]
                            for later in range(2)
                        ],
                        axis=1,
                    )
                    for kind in (b, batch, batch + 1)
                    for parity in range(2)
                ],
                axis=0,
            ).astype(jnp.bfloat16)
            right = jnp.concatenate(
                [
                    hankel[(4 * inner + half) * window : (4 * inner + half) * window + BLOCK, :]
                    for half in range(HALVES)
                ],
                axis=1,
            )
            term = product(left, right)
            result = term if result is None else result + term
        for parity in range(2):
            shared = result[parity * height : (parity + 1) * height]
            high = result[(2 + parity) * height : (3 + parity) * height]
            low = result[(4 + parity) * height : (5 + parity) * height]
            for half in range(HALVES):
                lanes = slice(half * LANES, (half + 1) * LANES)
                total[batch, parity, half, 0:height, :] += shared[:, lanes]
                if group == 0 and part == 0:
                    total[b, parity, half, 0:height, :] = high[:, lanes] + low[:, lanes]
                    total[b, parity, half, height : blocks + ROWS, :] = jnp.zeros(
                        (blocks + ROWS - height, LANES), jnp.float32
                    )
                else:
                    total[b, parity, half, 0:height, :] += high[:, lanes] + low[:, lanes]

    build(0, 0, even)
    lower = lax.broadcasted_iota(jnp.int32, (blocks, LANES), 1) < per_batch
    taps = [
        jnp.where(lower, rows_of(2 * half, SENT - 1), rows_of(2 * half + 1, SENT - 1))
        for half in range(HALVES)
    ]
    high = [half.astype(jnp.bfloat16).astype(jnp.float32) for half in taps]
    put_in_order(batch, high)
    put_in_order(batch + 1, [half - part for half, part in zip(taps, high)])
    for b in range(batch):
        put_in_order(b, [rows_of(b, half) for half in range(HALVES)])
    total[batch] = jnp.zeros(total.shape[1:], jnp.float32)

    def one_batch(b, last):
        for group in range(groups):
            now, later = (even, odd) if group % 2 == 0 else (odd, even)
            if group + 1 < groups:
                build(b, group + 1, later)
            elif not last:
                build(b + 1, 0, later)
            for part in range(PACK // ROWS):
                multiply(b, group, part, now)

    for b in range(batch):
        one_batch(b, b == batch - 1)

    last_lane = lax.broadcasted_iota(jnp.int32, (blocks, LANES), 1) == LANES - 1
    for kind in range(batch + 1):
        late = [pltpu.roll(total[kind, 1, half, 0:blocks, :], LANES - 1, 1) for half in range(HALVES)]
        late.append(pltpu.roll(total[kind, 1, 0, 1 : blocks + 1, :], LANES - 1, 1))
        for half in range(HALVES):
            joined = total[kind, 0, half, 0:blocks, :] + jnp.where(
                last_lane, late[half + 1], late[half]
            )
            if kind < batch:
                joined = joined + gain * rows_of(kind, HALVES + half)
                out_ref[pl.ds(kind * blocks * BACK + half, blocks, stride=BACK), :] = joined
            else:
                for b in range(half, batch, HALVES):
                    out_ref[pl.ds(b * blocks * BACK + HALVES, blocks, stride=BACK), :] = joined


def correlations(got, batch, blocks):
    hankel = pltpu.VMEM(((2 * PACK + 3) * LANES // 2, LANES), jnp.bfloat16)
    return pl.pallas_call(
        functools.partial(correlate, batch, blocks),
        out_shape=jax.ShapeDtypeStruct((batch * blocks * BACK, LANES), jnp.float32),
        in_specs=[pl.BlockSpec(memory_space=pltpu.VMEM)],
        out_specs=pl.BlockSpec(memory_space=pltpu.VMEM),
        scratch_shapes=[
            hankel,
            hankel,
            pltpu.VMEM((batch + 2, 2, blocks + PACK, LANES), jnp.float32),
            pltpu.VMEM((batch + 1, 2, HALVES, blocks + ROWS, LANES), jnp.float32),
        ],
        compiler_params=pltpu.CompilerParams(vmem_limit_bytes=24 * 1024 * 1024),
        cost_estimate=pl.CostEstimate(flops=6_000_000_000, bytes_accessed=2_000_000, transcendentals=0),
        name="correlate",
    )(got)


def write_out(pairs, left):
    copies = [
        pltpu.make_async_copy(source, target, left.at[place])
        for place, (source, target) in enumerate(pairs)
    ]
    for copy in copies:
        copy.start()
    return copies


def turn(home_ref, half_ref):
    channels = half_ref.shape[1]
    half_ref[...] = home_ref[pl.ds(HALVES, channels, stride=BACK), :].T


def filter_half(home):
    channels = home.shape[0] // BACK
    vmem = pl.BlockSpec(memory_space=pltpu.VMEM)
    return pl.pallas_call(
        turn,
        out_shape=jax.ShapeDtypeStruct((LANES, channels), jnp.float32),
        in_specs=[vmem],
        out_specs=vmem,
        compiler_params=pltpu.CompilerParams(vmem_limit_bytes=16 * 1024 * 1024),
        name="turn",
    )(home)


def finish(home_ref, input_ref, own, left):
    channels = input_ref.shape[2]
    copies = []
    for half in range(HALVES):
        rows = slice(half * LANES, (half + 1) * LANES)
        conv = home_ref[pl.ds(half, channels, stride=BACK), :].T
        own[0, rows, :] = conv.astype(jnp.bfloat16)
        copies += write_out([(own.at[:, rows, :], input_ref.at[:, rows, :])], left.at[pl.ds(half, 1)])
    for copy in copies:
        copy.wait()


def input_gradient(home):
    channels = home.shape[0] // BACK
    return pl.pallas_call(
        finish,
        out_shape=jax.ShapeDtypeStruct((1, BLOCK, channels), jnp.bfloat16),
        in_specs=[pl.BlockSpec(memory_space=pltpu.VMEM)],
        out_specs=pl.BlockSpec(memory_space=pltpu.HBM),
        scratch_shapes=[
            pltpu.VMEM((1, BLOCK, channels), jnp.bfloat16),
            pltpu.SemaphoreType.DMA((HALVES,)),
        ],
        compiler_params=pltpu.CompilerParams(vmem_limit_bytes=16 * 1024 * 1024),
        cost_estimate=pl.CostEstimate(flops=1_000_000_000, bytes_accessed=1_000_000, transcendentals=0),
        name="finish",
    )(home)


def join(own_ref, other_ref, filter_ref, left):
    core = lax.rem(lax.axis_index("batch"), HALVES)
    copies = write_out(
        [
            (own_ref, filter_ref.at[pl.ds(pl.multiple_of(core * LANES, LANES), LANES), :]),
            (other_ref, filter_ref.at[pl.ds(pl.multiple_of((1 - core) * LANES, LANES), LANES), :]),
        ],
        left,
    )
    for copy in copies:
        copy.wait()


def filter_gradient(own, other):
    vmem = pl.BlockSpec(memory_space=pltpu.VMEM)
    return pl.pallas_call(
        join,
        out_shape=jax.ShapeDtypeStruct((BLOCK, own.shape[1]), jnp.float32),
        in_specs=[vmem, vmem],
        out_specs=pl.BlockSpec(memory_space=pltpu.HBM),
        scratch_shapes=[pltpu.SemaphoreType.DMA((HALVES,))],
        compiler_params=pltpu.CompilerParams(vmem_limit_bytes=16 * 1024 * 1024),
        name="join",
    )(own, other)


def shards(signal, grad_out, filter_taps, skip_gain):
    batch, blocks = lax.axis_size("batch"), lax.axis_size("seq")
    axes = ("batch", "seq")
    channels = filter_taps.shape[1]
    grad_rows = grad_out[0].astype(jnp.float32)
    signal_rows = signal[0].astype(jnp.float32)
    per_batch = BLOCK // batch
    gain = jnp.broadcast_to(skip_gain[None, :], (LANES - per_batch, channels))
    signal_rows, grad_rows, gain = lax.optimization_barrier((signal_rows, grad_rows, gain))
    sent = pieces_to_send(signal_rows, grad_rows, filter_taps, gain, per_batch)
    sent = sent.reshape(channels, SENT, 1, LANES)
    got = lax.all_to_all(sent, axes, 0, 0, tiled=True)
    back = correlations(got.reshape(channels * SENT, LANES), batch, blocks)
    home = lax.all_to_all(back.reshape(channels, BACK, 1, LANES), axes, 0, 0, tiled=True)
    home = home.reshape(channels * BACK, LANES)
    own = filter_half(home)
    other = lax.ppermute(own, "batch", [(b, b ^ 1) for b in range(batch)])
    return (input_gradient(home), filter_gradient(own, other))


def solution(mesh):
    return jax.shard_map(
        shards,
        mesh=mesh,
        in_specs=(P("batch", "seq", None), P("batch", "seq", None), P("seq", None), P()),
        out_specs=(P("batch", "seq", None), P("seq", None)),
        check_vma=False,
    )
```
